32 devices in a mesh: win: 32 (over z, y, x, core).
Axes of the slice: x: 2, y: 2, z: 4, core: 2. Of those that a mesh axis runs over, the one named last changes fastest.
Arguments:
- point_rows: int32 [64, 32768], P('win'), may hold values from 0 to 31
- point_cols: int32 [64, 32768], P('win'), may hold values from 0 to 1023
- point_chans: int32 [64, 32768], P('win'), may hold values from 0 to 3
- point_weights: bfloat16 [64, 32768], P('win'), may hold values from 0.25 to 4
- decay: float32 [64, 4], P('win'), may hold values from 0.3 to 1
Outputs:
- heat: float32 [64, 4, 32, 1024], P('win')
The draws below stay inside these ranges and needn't reach their ends.
All inputs are finite; a program needn't handle non-finite values.
Results may differ from the reference program's by a relative error of at most 0.0003.
Values sent between devices are 32-bit elements; how exact they have to be, the bound alone decides.
A program may use at most 64 MiB of HBM per device.

```python
import math
import jax
import jax.numpy as jnp
import numpy as np
from jax import lax

IMAGE_LAYERS = 4
COLS = 1024
ROWS = 32
P_DEV = 32768
PERIOD_COUNT = 64


def draw_decay(key, part):
    generator_seeds = jax.random.split(jax.random.fold_in(key, 77), 6)
    order = jax.random.permutation(generator_seeds[0], IMAGE_LAYERS)
    slow = order < IMAGE_LAYERS // 2
    slow_rate = jax.random.uniform(generator_seeds[1], (IMAGE_LAYERS,), jnp.float32, 0.2, 1.0) / PERIOD_COUNT
    fast_rate = 1.0 / jax.random.uniform(generator_seeds[2], (IMAGE_LAYERS,), jnp.float32, 8.0, 20.0)
    base = jnp.where(slow, slow_rate, fast_rate)
    jitter = jax.random.uniform(generator_seeds[3], (PERIOD_COUNT, IMAGE_LAYERS), jnp.float32, 0.5, 2.0)
    sudden_surge = jax.random.uniform(generator_seeds[4], (PERIOD_COUNT, IMAGE_LAYERS), jnp.float32) < 3.0 / PERIOD_COUNT
    fading_multiplier = jnp.where(sudden_surge, jax.random.uniform(generator_seeds[5], (PERIOD_COUNT, IMAGE_LAYERS), jnp.float32, 0.5, 0.8), 1.0)
    return (jnp.exp(-base[None, :] * jitter) * fading_multiplier).astype(jnp.float32)


def touch_ends(result, key, low, top_value):
    spot = [jax.random.randint(jax.random.fold_in(key, axis), (), 0, length) for axis, length in enumerate(result.shape)]
    main_axis = result.shape.index(max(result.shape))
    beside = spot[:main_axis] + [(spot[main_axis] + 1) % result.shape[main_axis]] + spot[main_axis + 1:]
    return result.at[tuple(spot)].set(low).at[tuple(beside)].set(top_value)


def block_levels(own_key, shape, pieces, low, high):
    def one(position, parts):
        draws = jax.random.uniform(jax.random.fold_in(jax.random.fold_in(own_key, 6), position), (parts,), jnp.float32, low / len(pieces), high / len(pieces))
        return jnp.repeat(jnp.exp(draws), shape[position] // parts).reshape((-1,) + (1,) * (len(shape) - position - 1))

    gain = one(*pieces[0])
    for cut in pieces[1:]:
        gain = gain * one(*cut)
    return gain


def cumulative_ranks(amount, slope):
    loads = [(1 << 20) // math.isqrt(grade ** slope) + 1 for grade in range(1, amount + 1)]
    width = 1 + sum(loads) // (1 << 30)
    return np.cumsum(np.array([max(1, weight // width) for weight in loads]))


def ranked(key, extent, number_of, skew):
    listing = cumulative_ranks(number_of, skew)
    pick = jax.random.randint(jax.random.fold_in(key, 1), extent, 0, int(listing[number_of - 1]))
    standing = jnp.searchsorted(jnp.asarray(listing, jnp.int32), pick, side="right")
    return jax.random.permutation(jax.random.fold_in(key, 2), number_of)[standing].astype(jnp.int32)


def setup_inputs(seed: int = 0) -> dict:
    arg_keys = jax.random.split(jax.random.key(seed), 6)
    point_rows = touch_ends(jax.random.randint(arg_keys[0], (PERIOD_COUNT, P_DEV), 0, ROWS), jax.random.fold_in(arg_keys[0], 1), 0, ROWS - 1).astype(jnp.int32)
    point_cols = touch_ends(ranked(arg_keys[1], (PERIOD_COUNT, P_DEV), COLS, 1), jax.random.fold_in(arg_keys[1], 3), 0, COLS - 1).astype(jnp.int32)
    point_chans = touch_ends(jax.random.randint(arg_keys[2], (PERIOD_COUNT, P_DEV), 0, IMAGE_LAYERS), jax.random.fold_in(arg_keys[2], 1), 0, IMAGE_LAYERS - 1).astype(jnp.int32)
    point_weights = jnp.clip(jnp.exp(math.log(4.0) - 2.7725887 * jax.random.uniform(arg_keys[3], (PERIOD_COUNT, P_DEV), jnp.float32) ** block_levels(arg_keys[3], (PERIOD_COUNT, P_DEV), ((0, 32),), -0.2, 0.2)), 0.25, 4.0).astype(jnp.bfloat16)
    decay = draw_decay(jax.random.fold_in(arg_keys[5], 71), 0)
    return {"point_rows": point_rows, "point_cols": point_cols, "point_chans": point_chans, "point_weights": point_weights, "decay": decay}


def reference(point_rows, point_cols, point_chans, point_weights, decay):
    flattened_index = (point_chans * ROWS + point_rows) * COLS + point_cols
    windows = point_rows.shape[0]
    window_ids = jnp.arange(windows, dtype=jnp.int32)[:, None] + jnp.zeros_like(flattened_index)
    hist = jnp.zeros((windows, IMAGE_LAYERS * ROWS * COLS), jnp.float32)
    hist = hist.at[window_ids, flattened_index].add(point_weights.astype(jnp.float32))
    hist = hist.reshape(windows, IMAGE_LAYERS, ROWS, COLS)

    def advance(carry, input_arrays):
        fading_multiplier, canvas = input_arrays
        carry = fading_multiplier[:, None, None] * carry + canvas
        return carry, carry

    start = jnp.zeros((IMAGE_LAYERS, ROWS, COLS), jnp.float32)
    final, heat = lax.scan(advance, start, (decay, hist))
    return heat
```

```python
import functools
import jax, jax.numpy as jnp
from jax import lax
from jax.experimental import pallas as pl
from jax.experimental.pallas import tpu as pltpu
from jax.sharding import PartitionSpec as P
IMAGE_LAYERS=4
SLOTS=128; ROWS=32; COLS=1024; PART=256; LANES=128; SUB=8
PARTS=2
UNROLL=8
def hot(index, on):
    spread = jnp.broadcast_to(index, (16, LANES)).astype(jnp.bfloat16)
    slots = lax.broadcasted_iota(jnp.int32, (16, LANES), 0).astype(jnp.float32).astype(jnp.bfloat16)
    off = jnp.zeros((16, LANES), jnp.bfloat16)
    return jnp.concatenate([jnp.where(spread == slots + jnp.bfloat16(16.0*g), on, off) for g in range(16)], axis=0)

def swap(x, bits):
    sub = lax.broadcasted_iota(jnp.int32, (SUB, LANES), 0)
    return jnp.take_along_axis(x, sub ^ bits, axis=0)

def exchange(xs, i, j):
    xs[i], xs[j] = jnp.minimum(xs[i], xs[j]), jnp.maximum(xs[i], xs[j])

def sort_rows(xs):
    n=len(xs); xs=list(xs)
    sub = lax.broadcasted_iota(jnp.int32, (SUB, LANES), 0)
    k=2
    while k<=n:
        for b in range(0,n,k):
            for t in range(k//2): exchange(xs,b+t,b+k-1-t)
        d=k//4
        while d:
            for i in range(n):
                if not i & d: exchange(xs,i,i+d)
            d//=2
        k*=2
    width=1
    while width<SUB:
        low = (sub & width)==0
        ys=[swap(x,2*width-1) for x in xs]
        xs=[jnp.where(low,jnp.minimum(xs[i],ys[n-1-i]),jnp.maximum(xs[i],ys[n-1-i])) for i in range(n)]
        d=width//2
        while d:
            low=(sub & d)==0
            xs=[jnp.where(low,jnp.minimum(x,y),jnp.maximum(x,y)) for x,y in ((x,swap(x,d)) for x in xs)]
            d//=2
        d=n//2
        while d:
            for i in range(n):
                if not i & d: exchange(xs,i,i+d)
            d//=2
        width*=2
    return xs

def kernel(rows_hbm, cols_hbm, chans_hbm, weights_hbm, decay_hbm, out, fact, rows, cols, chans, weights, decay, keys, place, where_, weigh, sem):
    copies=[pltpu.make_async_copy(a,b,sem.at[i]) for i,(a,b) in enumerate(((decay_hbm,decay),(weights_hbm,weights),(cols_hbm,cols),(chans_hbm,chans),(rows_hbm,rows)))]
    for copy in copies: copy.start()
    for copy in copies: copy.wait()
    pl.run_scoped(functools.partial(bin_points,rows,cols,chans,weights,decay,out,fact,keys,place,where_,weigh),
        pltpu.ACC(0)((256,256),jnp.float32),pltpu.ACC(1)((256,256),jnp.float32))

def bin_points(rows, cols, chans, weights, decay, out, fact, keys, place, where_, weigh, *accs):
    windows = out.shape[0]
    for channel in range(IMAGE_LAYERS):
        factor = jnp.float32(1.0)
        for w in range(windows):
            factor = factor * decay[w, channel]
            fact[w, channel : channel + 1, :] = jnp.full((1, LANES), factor, jnp.float32)
    total = rows.shape[0]; height = total//windows
    for a in accs: out[0,:,0:256]=pltpu.matmul_pop(a)[:128]
    for v in range(total//16):
        at=pl.ds(16*v,16)
        c=cols[at,:]; k=chans[at,:]
        w=(weights[at,:].astype(jnp.float32)*512.0).astype(jnp.int32)
        lidx=((k>>1)<<8)|((c>>8)<<6)|((k&1)<<5)|rows[at,:]
        keys[at,:]=(lidx<<20)|((c&255)<<12)|w
    bounds=[]
    n=height//SUB
    for w in range(windows):
        xs=[keys[pl.ds(w+windows*SUB*v,SUB,stride=windows),:] for v in range(n)]
        xs=sort_rows(xs)
        first=jnp.zeros((SUB,LANES),jnp.int32)
        for v in range(n):
            x=xs[v]
            first=first+jnp.where(x<(1<<28),1,0)
            at=pl.ds(v,SUB,stride=n)
            place[w,at,:]=(x>>20).astype(jnp.float32)
            where_[w,at,:]=((x>>12)&255).astype(jnp.float32)
            weigh[w,at,:]=(x&4095).astype(jnp.float32)*(1.0/512.0)
        first=jnp.sum(first,axis=0,keepdims=True)
        bounds.append((jnp.min(first),jnp.max(first)))
    one=jnp.ones((16,LANES),jnp.bfloat16)
    step=2*UNROLL
    def right(w,r):
        return jnp.concatenate([hot(where_[w,pl.ds(r+i,1),:],jnp.broadcast_to(weigh[w,pl.ds(r+i,1),:],(16,LANES)).astype(jnp.bfloat16)) for i in range(2)],axis=1)
    def left(w,r,base):
        return jnp.concatenate([hot(place[w,pl.ds(r+i,1),:]-base,one) for i in range(2)],axis=1)
    for w in range(windows):
        for p in range(PARTS):
            lo,hi=bounds[w]
            if p==0:
                begin=jnp.int32(0); trips=(hi+step-1)//step
            else:
                begin=(lo//step)*step; trips=(height-begin)//step
            for m in range(2):
                pltpu.matmul_push_rhs(right(w,begin+2*m),staging_register=0,mxu_index=m,transpose=True)
            def body(i,c):
                base_r=begin+i*step
                for u in range(UNROLL):
                    m=u%2; s=(u//2)%2
                    r=base_r+2*u
                    nxt=r+4
                    if u>=UNROLL-2: nxt=jnp.minimum(nxt,height-2)
                    pltpu.matmul_push_rhs(right(w,nxt),staging_register=1-s,mxu_index=m,transpose=True)
                    pltpu.matmul_acc_lhs(accs[m],left(w,r,256.0*p),load_staged_rhs=s)
                return c
            lax.fori_loop(0,trips,body,0)
            for m in range(2):
                pltpu.matmul_acc_lhs(accs[m],jnp.zeros((256,256),jnp.bfloat16),load_staged_rhs=0)
            got=pltpu.matmul_pop(accs[0])+pltpu.matmul_pop(accs[1])
            for j in range(4):
                for c in range(2):
                    at=slice(64*p+32*c,64*p+32*c+32)
                    piece=got[64*j+32*c:64*j+32*c+32]
                    if w: piece=decay[w,2*p+c]*out[w-1,at,256*j:256*j+256]+piece
                    out[w,at,256*j:256*j+256]=piece
def view(x):
    windows,count=x.shape
    return x.reshape(windows,count//LANES,LANES).transpose(1,0,2).reshape(windows*count//LANES,LANES)
def binned(r,c,k,w,d):
    windows,count=r.shape
    height=count//LANES
    tall=windows*height
    return pl.pallas_call(
        kernel,
        out_shape=(
            jax.ShapeDtypeStruct((windows, SLOTS, COLS), jnp.float32),
            jax.ShapeDtypeStruct((windows, SUB, LANES), jnp.float32),
        ),
        in_specs=[pl.BlockSpec(memory_space=pltpu.HBM)] * 5,
        out_specs=[pl.BlockSpec(memory_space=pltpu.VMEM)] * 2,
        scratch_shapes=[pltpu.VMEM((tall, LANES), jnp.int32)] * 3
        + [pltpu.VMEM((tall, LANES), jnp.bfloat16), pltpu.SMEM(d.shape, jnp.float32)]
        + [pltpu.VMEM((tall, LANES), jnp.int32)]
        + [pltpu.VMEM((windows, height, LANES), jnp.float32)] * 3
        + [pltpu.SemaphoreType.DMA((5,))],
        compiler_params=pltpu.CompilerParams(vmem_limit_bytes=16 * 2**20),
    )(*(pltpu.with_memory_space_constraint(x, pltpu.HBM) for x in (*map(view, (r, c, k, w)), d)))


MESH = pl.DeviceIdType.MESH
CHUNK = 512


def across(tile):
    return jnp.concatenate([tile] * (CHUNK // LANES), axis=1)


def scan_kernel(
    n, size, running_hbm, fact_ref, out_ref,
    own, other, stage, inbox, total, earlier, carried, spread, back, prefix, handed, received,
    load_sem, swap_send, swap_recv, go_send, go_recv, up_send, up_recv, back_send, back_recv, hand_send, hand_recv,
):
    windows = running_hbm.shape[0]
    groups, chips = n // size, size // 2
    half = SLOTS // 2
    piece = half // chips
    chunks = COLS // CHUNK
    me = lax.axis_index("win")
    group, member = lax.div(me, size), lax.rem(me, size)
    chip, side = lax.div(member, 2), lax.rem(member, 2)
    partner = me + 1 - 2 * side
    mate = lambda k: group * size + 2 * lax.rem(chip + k, chips) + side
    counter = lambda k: lax.rem(me + k * size, n)

    barrier = pltpu.get_barrier_semaphore()
    peers = [partner] + [mate(k) for k in range(1, chips)] + [counter(k) for k in range(1, groups)]
    for peer in peers:
        pl.semaphore_signal(barrier, inc=1, device_id=(peer,), device_id_type=MESH)
    for c in range(chunks):
        own[c, :, :CHUNK] = running_hbm[windows - 1, :, c * CHUNK : (c + 1) * CHUNK]
    for channel in range(IMAGE_LAYERS):
        factor = fact_ref[windows - 1, channel : channel + 1, :]
        own[0, channel * ROWS : (channel + 1) * ROWS, CHUNK:] = jnp.broadcast_to(factor, (ROWS, LANES))

    def sent(ref, chunk):
        return ref if chunk == 0 else ref.at[:, pl.ds(0, CHUNK)]

    def remote(src, dst, send, recv, device):
        return pltpu.make_async_remote_copy(
            src_ref=src, dst_ref=dst, send_sem=send, recv_sem=recv, device_id=(device,), device_id_type=MESH
        )

    def swap_sides(chunk):
        away = own.at[chunk, pl.ds(pl.multiple_of((1 - side) * half, half), half)]
        return remote(
            sent(away, chunk), sent(other.at[chunk], chunk), swap_send.at[chunk], swap_recv.at[chunk], partner
        )

    def go(chunk, k, sender):
        peer = lax.rem(chip + k, chips)
        slot = chip if sender else peer
        return remote(
            sent(stage.at[chunk, peer], chunk), sent(inbox.at[chunk, slot], chunk),
            go_send.at[chunk, k], go_recv.at[chunk, slot], mate(k),
        )

    def up(chunk, k, slot):
        return remote(
            sent(total.at[chunk], chunk), sent(earlier.at[chunk, slot], chunk),
            up_send.at[chunk, k], up_recv.at[chunk, slot], counter(k),
        )

    def give(chunk, k, sender):
        peer = lax.rem(chip + k, chips)
        slot = chip if sender else peer
        return remote(
            back.at[chunk, peer], prefix.at[chunk, slot], back_send.at[chunk, k], back_recv.at[chunk, slot], mate(k)
        )

    def hand(chunk):
        return remote(
            handed.at[chunk], received.at[chunk], hand_send.at[chunk], hand_recv.at[chunk], partner
        )

    first = side == 0
    mine_at = pl.ds(pl.multiple_of(side * half, half), half)

    def combine(chunk):
        swap_sides(chunk).wait_recv()
        a, b = own[chunk, mine_at, :CHUNK], other[chunk, :, :CHUNK]
        fa, fb = own[0, mine_at, CHUNK:], other[0, :, CHUNK:]
        late = across(jnp.where(first, fb, fa))
        both = late * jnp.where(first, a, b) + jnp.where(first, b, a)
        for p in range(chips):
            stage[chunk, p, :, :CHUNK] = both[p * piece : (p + 1) * piece]
            if chunk == 0:
                stage[chunk, p, :, CHUNK:] = (fa * fb)[p * piece : (p + 1) * piece]
        for k in range(1, chips):
            go(chunk, k, True).start()
        wide = CHUNK if chunk else CHUNK + LANES
        inbox[chunk, chip, :, :wide] = stage[chunk, chip, :, :wide]

    def give_all(chunk):
        for k in range(1, chips):
            give(chunk, k, True).start()
        prefix[chunk, chip] = back[chunk, chip]

    def scan_group(chunk):
        for k in range(1, chips):
            go(chunk, k, False).wait_recv()
        running = jnp.zeros((piece, CHUNK), jnp.float32)
        factor = jnp.ones((piece, LANES), jnp.float32)
        for m in range(chips):
            back[chunk, m] = running
            by = inbox[0, m, :, CHUNK:]
            if chunk == 0:
                spread[m] = factor
            running = across(by) * running + inbox[chunk, m, :, :CHUNK]
            if chunk == 0:
                factor = factor * by
        total[chunk, :, :CHUNK] = running
        if chunk == 0:
            total[chunk, :, CHUNK:] = factor
        for k in range(1, groups):

            @pl.when(group + k < groups)
            def _():
                up(chunk, k, group).start()

        @pl.when(group == 0)
        def _():
            give_all(chunk)

    def finish_groups(chunk):
        if groups == 1:
            return
        carried[...] = jnp.zeros((piece, CHUNK), jnp.float32)
        for g in range(groups - 1):

            @pl.when(g < group)
            def _():
                up(chunk, 1, g).wait_recv()
                by = earlier[0, g, :, CHUNK:]
                carried[...] = across(by) * carried[...] + earlier[chunk, g, :, :CHUNK]

        @pl.when(group > 0)
        def _():
            before = carried[...]
            for m in range(chips):
                back[chunk, m] += across(spread[m]) * before
            give_all(chunk)

    def pass_on(chunk):
        for k in range(1, chips):
            give(chunk, k, False).wait_recv()
        before = prefix[chunk].reshape(half, CHUNK)
        a, b = own[chunk, mine_at, :CHUNK], other[chunk, :, :CHUNK]
        fa, fb = own[0, mine_at, CHUNK:], other[0, :, CHUNK:]
        after = across(jnp.where(first, fa, fb)) * before + jnp.where(first, a, b)
        handed[chunk] = jnp.where(first, after, before)
        hand(chunk).start()
        out_ref[mine_at, chunk * CHUNK : (chunk + 1) * CHUNK] = jnp.where(first, before, after)

    def take(chunk):
        hand(chunk).wait_recv()
        at = pl.ds(pl.multiple_of((1 - side) * half, half), half)
        out_ref[at, chunk * CHUNK : (chunk + 1) * CHUNK] = received[chunk]

    for chunk in range(chunks):
        if chunk == 0:
            pl.semaphore_wait(barrier, len(peers))
        swap_sides(chunk).start()
    for chunk in range(chunks):
        combine(chunk)
    for chunk in range(chunks):
        scan_group(chunk)
    for chunk in range(chunks):
        finish_groups(chunk)
    for chunk in range(chunks):
        pass_on(chunk)
    for chunk in range(chunks):
        take(chunk)

    for chunk in range(chunks):
        swap_sides(chunk).wait_send()
        hand(chunk).wait_send()
        for k in range(1, chips):
            go(chunk, k, True).wait_send()
            give(chunk, k, True).wait_send()
        for k in range(1, groups):

            @pl.when(group + k < groups)
            def _():
                up(chunk, k, group).wait_send()


def before_own(n, running, fact):
    size = max(s for s in range(2, 2 * SLOTS // (2 * SUB) + 1, 2) if n % s == 0 and SLOTS % (s * SUB) == 0)
    groups, chips = n // size, size // 2
    half = SLOTS // 2
    piece, chunks = half // chips, COLS // CHUNK
    wide = CHUNK + LANES
    dma = pltpu.SemaphoreType.DMA
    f32 = lambda *shape: pltpu.VMEM(shape, jnp.float32)
    return pl.pallas_call(
        functools.partial(scan_kernel, n, size),
        out_shape=jax.ShapeDtypeStruct((SLOTS, COLS), jnp.float32),
        in_specs=[pl.BlockSpec(memory_space=pltpu.VMEM)] * 2,
        out_specs=pl.BlockSpec(memory_space=pltpu.VMEM),
        scratch_shapes=[
            f32(chunks, SLOTS, wide), f32(chunks, half, wide), f32(chunks, chips, piece, wide),
            f32(chunks, chips, piece, wide), f32(chunks, piece, wide), f32(chunks, groups, piece, wide),
            f32(piece, CHUNK), f32(chips, piece, LANES), f32(chunks, chips, piece, CHUNK),
            f32(chunks, chips, piece, CHUNK), f32(chunks, half, CHUNK), f32(chunks, half, CHUNK),
            dma((chunks,)), dma((chunks,)), dma((chunks,)), dma((chunks, chips)), dma((chunks, chips)),
            dma((chunks, groups)), dma((chunks, groups)), dma((chunks, chips)), dma((chunks, chips)),
            dma((chunks,)), dma((chunks,)),
        ],
        compiler_params=pltpu.CompilerParams(collective_id=0, has_side_effects=True, vmem_limit_bytes=16 * 2**20),
    )(running, fact)


def heat_kernel(running_ref, before_ref, fact_ref, out_hbm, out_ref, sem):
    windows = running_ref.shape[0]
    stores = []
    for channel in range(IMAGE_LAYERS):
        at = slice(channel * ROWS, (channel + 1) * ROWS)
        for window in range(windows):
            factor = jnp.concatenate([fact_ref[window, channel : channel + 1, :]] * (COLS // LANES), axis=1)
            out_ref[window, at] = factor * before_ref[at] + running_ref[window, at]
            stores.append(
                pltpu.make_async_copy(out_ref.at[window, at], out_hbm.at[window, at], sem.at[window, channel])
            )
            stores[-1].start()
    for store in stores:
        store.wait()


def heat(running, before, fact):
    windows = running.shape[0]
    return pl.pallas_call(
        heat_kernel,
        out_shape=jax.ShapeDtypeStruct(running.shape, jnp.float32),
        in_specs=[pl.BlockSpec(memory_space=pltpu.VMEM)] * 3,
        out_specs=pl.BlockSpec(memory_space=pltpu.HBM),
        scratch_shapes=[pltpu.VMEM(running.shape, jnp.float32), pltpu.SemaphoreType.DMA((windows, IMAGE_LAYERS))],
        compiler_params=pltpu.CompilerParams(vmem_limit_bytes=8 * 2**20),
    )(running, before, fact)


def local(n, point_rows, point_cols, point_chans, point_weights, decay):
    running, fact = binned(point_rows, point_cols, point_chans, point_weights, decay)
    before = before_own(n, running, fact)
    return heat(running, before, fact).reshape(-1, IMAGE_LAYERS, ROWS, COLS)


def solution(mesh):
    placed = (P("win", None),) * 5
    return jax.shard_map(
        functools.partial(local, mesh.shape["win"]),
        mesh=mesh, in_specs=placed, out_specs=P("win", None, None, None), check_vma=False,
    )
```

```python
import functools
import jax, jax.numpy as jnp
from jax import lax
from jax.experimental import pallas as pl
from jax.experimental.pallas import tpu as pltpu
from jax.sharding import PartitionSpec as P
IMAGE_LAYERS=4
SLOTS=128; ROWS=32; COLS=1024; PART=256; LANES=128; SUB=8
PARTS=2
UNROLL=8
STEP=2*UNROLL
PAD=STEP
MIDDLE=64
def hot(index, on):
    spread = jnp.broadcast_to(index, (16, LANES)).astype(jnp.bfloat16)
    slots = lax.broadcasted_iota(jnp.int32, (16, LANES), 0).astype(jnp.float32).astype(jnp.bfloat16)
    off = jnp.zeros((16, LANES), jnp.bfloat16)
    return jnp.concatenate([jnp.where(spread == slots + jnp.bfloat16(16.0*g), on, off) for g in range(16)], axis=0)

def swap(x, bits):
    sub = lax.broadcasted_iota(jnp.int32, (SUB, LANES), 0)
    return jnp.take_along_axis(x, sub ^ bits, axis=0)

def exchange(xs, i, j):
    xs[i], xs[j] = jnp.minimum(xs[i], xs[j]), jnp.maximum(xs[i], xs[j])

def sort_rows(xs):
    n=len(xs); xs=list(xs)
    sub = lax.broadcasted_iota(jnp.int32, (SUB, LANES), 0)
    k=2
    while k<=n:
        for b in range(0,n,k):
            for t in range(k//2): exchange(xs,b+t,b+k-1-t)
        d=k//4
        while d:
            for i in range(n):
                if not i & d: exchange(xs,i,i+d)
            d//=2
        k*=2
    width=1
    while width<SUB:
        low = (sub & width)==0
        ys=[swap(x,2*width-1) for x in xs]
        xs=[jnp.where(low,jnp.minimum(xs[i],ys[n-1-i]),jnp.maximum(xs[i],ys[n-1-i])) for i in range(n)]
        d=width//2
        while d:
            low=(sub & d)==0
            xs=[jnp.where(low,jnp.minimum(x,y),jnp.maximum(x,y)) for x,y in ((x,swap(x,d)) for x in xs)]
            d//=2
        d=n//2
        while d:
            for i in range(n):
                if not i & d: exchange(xs,i,i+d)
            d//=2
        width*=2
    return xs

def kernel(rows_hbm, cols_hbm, chans_hbm, weights_hbm, decay_hbm, out, fact, rows, cols, chans, weights, decay, keys, place, where_, weigh, ahead, sem):
    copies=[pltpu.make_async_copy(a,b,sem.at[i]) for i,(a,b) in enumerate(((decay_hbm,decay),(weights_hbm,weights),(cols_hbm,cols),(chans_hbm,chans),(rows_hbm,rows)))]
    for copy in copies: copy.start()
    for copy in copies: copy.wait()
    pl.run_scoped(functools.partial(bin_points,rows,cols,chans,weights,decay,out,fact,keys,place,where_,weigh,ahead),
        *[pltpu.ACC(m)((256,256),jnp.float32) for _ in range(3) for m in range(2)])

def bin_points(rows, cols, chans, weights, decay, out, fact, keys, place, where_, weigh, ahead, *accs):
    windows = out.shape[0]
    for channel in range(IMAGE_LAYERS):
        factor = jnp.float32(1.0)
        for w in range(windows):
            factor = factor * decay[w, channel]
            fact[w, channel : channel + 1, :] = jnp.full((1, LANES), factor, jnp.float32)
    total = rows.shape[0]; height = total//windows
    for a in accs: out[0,:,0:256]=pltpu.matmul_pop(a)[:128]
    for v in range(total//16):
        at=pl.ds(16*v,16)
        c=cols[at,:]; k=chans[at,:]
        w=(weights[at,:].astype(jnp.float32)*512.0).astype(jnp.int32)
        lidx=((k>>1)<<8)|((c>>8)<<6)|((k&1)<<5)|rows[at,:]
        keys[at,:]=(lidx<<20)|((c&255)<<12)|w
    span=place.shape[0]//windows
    bounds=[]
    n=height//SUB
    for w in range(windows):
        xs=[keys[pl.ds(w+windows*SUB*v,SUB,stride=windows),:] for v in range(n)]
        xs=sort_rows(xs)
        counts=[jnp.zeros((SUB,LANES),jnp.int32) for _ in range(3)]
        for v in range(n):
            x=xs[v]
            for q in range(3):
                counts[q]=counts[q]+jnp.where(x<((q+1)<<27),1,0)
            at=pl.ds(w*span+PAD+v,SUB,stride=n)
            place[at,:]=(x>>20).astype(jnp.float32)
            where_[at,:]=((x>>12)&255).astype(jnp.float32)
            weigh[at,:]=(x&4095).astype(jnp.float32)*(1.0/512.0)
        for at in (slice(w*span,w*span+PAD),slice(w*span+PAD+height,(w+1)*span)):
            rest=(at.stop-at.start,LANES)
            place[at,:]=jnp.full(rest,-1000.0,jnp.float32)
            where_[at,:]=jnp.zeros(rest,jnp.float32)
            weigh[at,:]=jnp.zeros(rest,jnp.float32)
        low,mid,high=(jnp.sum(count,axis=0,keepdims=True) for count in counts)
        bounds.append((jnp.max(jnp.maximum(low,mid-MIDDLE)),jnp.min(jnp.minimum(mid,high-MIDDLE)),jnp.min(mid),jnp.max(mid)))
    one=jnp.ones((16,LANES),jnp.bfloat16)
    def right(r):
        return jnp.concatenate([hot(where_[pl.ds(r+i,1),:],jnp.broadcast_to(weigh[pl.ds(r+i,1),:],(16,LANES)).astype(jnp.bfloat16)) for i in range(2)],axis=1)
    def left(r,base):
        return jnp.concatenate([hot(place[pl.ds(r+i,1),:]-base,one) for i in range(2)],axis=1)
    def prepare(m,staging,r,base):
        pltpu.matmul_push_rhs(right(r),staging_register=staging,mxu_index=m,transpose=True)
        ahead[m]=left(r,base)
    def multiply(targets,begin,trips,base,then):
        def body(i,c):
            base_r=begin+i*STEP
            for u in range(UNROLL):
                m=u%2; s=(u//2)%2
                r=base_r+2*u
                nxt=r+4
                if u>=UNROLL-2: nxt=jnp.where(i==trips-1,then[0]+2*m,nxt)
                pltpu.matmul_push_rhs(right(nxt),staging_register=1-s,mxu_index=m,transpose=True)
                pltpu.matmul_acc_lhs(targets[m],ahead[m] if u<2 else left(r,base),load_staged_rhs=s)
                if u>=UNROLL-2: ahead[m]=left(nxt,jnp.where(i==trips-1,then[1],base))
            return c
        lax.fori_loop(0,trips,body,0)
    def put(w,got,quarter,blend):
        for block in range(8):
            index=4*quarter+block
            part,j,c=index//8,index//2%4,index%2
            at=slice(64*part+32*c,64*part+32*c+32)
            piece=got[32*block:32*block+32]
            out[w,at,256*j:256*j+256]=blend(out,w,at,j,2*part+c,piece)
    def begin_sum(out,w,at,j,channel,piece):
        return decay[w,channel]*out[w-1,at,256*j:256*j+256]+piece if w else piece
    def add(out,w,at,j,channel,piece):
        return out[w,at,256*j:256*j+256]+piece
    phases=[]
    for w in range(windows):
        least,most,lo,hi=bounds[w]
        split=least<=most
        a=jnp.clip(jnp.int32((height-MIDDLE)//2),least,most)
        up=lambda x: (x+STEP-1)//STEP
        trips=jnp.where(split,up(a),up(hi))
        phases.append((jnp.where(split,a-trips*STEP,0)+w*span+PAD,trips))
        phases.append((a+w*span+PAD,jnp.where(split,MIDDLE//STEP,0)))
        begin=jnp.where(split,a+MIDDLE,(lo//STEP)*STEP)
        phases.append((begin+w*span+PAD,up(height-begin)))
    starts=[(jnp.int32(0),jnp.float32(0.0))]
    for k in reversed(range(len(phases))):
        begin,trips=phases[k]
        some=trips>0
        starts.insert(0,(jnp.where(some,begin,starts[0][0]),jnp.where(some,jnp.float32(128.0*(k%3)),starts[0][1])))
    for m in range(2): prepare(m,0,starts[0][0]+2*m,starts[0][1])
    for w in range(windows):
        for p in range(3):
            begin,trips=phases[3*w+p]
            multiply(accs[2*p:2*p+2],begin,trips,jnp.float32(128.0*p),starts[3*w+p+1])
        for p,quarter in ((0,0),(2,2),(1,1)):
            put(w,pltpu.matmul_pop(accs[2*p])+pltpu.matmul_pop(accs[2*p+1]),quarter,add if p==1 else begin_sum)
    for m in range(2):
        pltpu.matmul_acc_lhs(accs[m],jnp.zeros((256,256),jnp.bfloat16),load_staged_rhs=0)
    out[0,:1,:256]=out[0,:1,:256]+(pltpu.matmul_pop(accs[0])+pltpu.matmul_pop(accs[1]))[:1]
def view(x):
    windows,count=x.shape
    return x.reshape(windows,count//LANES,LANES).transpose(1,0,2).reshape(windows*count//LANES,LANES)
def binned(r,c,k,w,d):
    windows,count=r.shape
    height=count//LANES
    tall=windows*height
    return pl.pallas_call(
        kernel,
        out_shape=(
            jax.ShapeDtypeStruct((windows, SLOTS, COLS), jnp.float32),
            jax.ShapeDtypeStruct((windows, SUB, LANES), jnp.float32),
        ),
        in_specs=[pl.BlockSpec(memory_space=pltpu.HBM)] * 5,
        out_specs=[pl.BlockSpec(memory_space=pltpu.VMEM)] * 2,
        scratch_shapes=[pltpu.VMEM((tall, LANES), jnp.int32)] * 3
        + [pltpu.VMEM((tall, LANES), jnp.bfloat16), pltpu.SMEM(d.shape, jnp.float32)]
        + [pltpu.VMEM((tall, LANES), jnp.int32)]
        + [pltpu.VMEM((windows * (PAD + height + PAD + SUB), LANES), jnp.float32)] * 3
        + [pltpu.VMEM((2, 256, 256), jnp.bfloat16)]
        + [pltpu.SemaphoreType.DMA((5,))],
        compiler_params=pltpu.CompilerParams(vmem_limit_bytes=16 * 2**20),
    )(*(pltpu.with_memory_space_constraint(x, pltpu.HBM) for x in (*map(view, (r, c, k, w)), d)))


MESH = pl.DeviceIdType.MESH
CHUNK = 512


def across(tile):
    return jnp.concatenate([tile] * (CHUNK // LANES), axis=1)


def scan_kernel(
    n, size, running_hbm, fact_ref, out_ref,
    own, other, stage, inbox, total, earlier, carried, spread, back, prefix, handed, received,
    load_sem, swap_send, swap_recv, go_send, go_recv, up_send, up_recv, back_send, back_recv, hand_send, hand_recv,
):
    windows = running_hbm.shape[0]
    groups, chips = n // size, size // 2
    half = SLOTS // 2
    piece = half // chips
    chunks = COLS // CHUNK
    me = lax.axis_index("win")
    group, member = lax.div(me, size), lax.rem(me, size)
    chip, side = lax.div(member, 2), lax.rem(member, 2)
    partner = me + 1 - 2 * side
    mate = lambda k: group * size + 2 * lax.rem(chip + k, chips) + side
    counter = lambda k: lax.rem(me + k * size, n)

    barrier = pltpu.get_barrier_semaphore()
    peers = [partner] + [mate(k) for k in range(1, chips)] + [counter(k) for k in range(1, groups)]
    for peer in peers:
        pl.semaphore_signal(barrier, inc=1, device_id=(peer,), device_id_type=MESH)
    for c in range(chunks):
        own[c, :, :CHUNK] = running_hbm[windows - 1, :, c * CHUNK : (c + 1) * CHUNK]
    for channel in range(IMAGE_LAYERS):
        factor = fact_ref[windows - 1, channel : channel + 1, :]
        own[0, channel * ROWS : (channel + 1) * ROWS, CHUNK:] = jnp.broadcast_to(factor, (ROWS, LANES))

    def sent(ref, chunk):
        return ref if chunk == 0 else ref.at[:, pl.ds(0, CHUNK)]

    def remote(src, dst, send, recv, device):
        return pltpu.make_async_remote_copy(
            src_ref=src, dst_ref=dst, send_sem=send, recv_sem=recv, device_id=(device,), device_id_type=MESH
        )

    def swap_sides(chunk):
        away = own.at[chunk, pl.ds(pl.multiple_of((1 - side) * half, half), half)]
        return remote(
            sent(away, chunk), sent(other.at[chunk], chunk), swap_send.at[chunk], swap_recv.at[chunk], partner
        )

    def go(chunk, k, sender):
        peer = lax.rem(chip + k, chips)
        slot = chip if sender else peer
        return remote(
            sent(stage.at[chunk, peer], chunk), sent(inbox.at[chunk, slot], chunk),
            go_send.at[chunk, k], go_recv.at[chunk, slot], mate(k),
        )

    def up(chunk, k, slot):
        return remote(
            sent(total.at[chunk], chunk), sent(earlier.at[chunk, slot], chunk),
            up_send.at[chunk, k], up_recv.at[chunk, slot], counter(k),
        )

    def give(chunk, k, sender):
        peer = lax.rem(chip + k, chips)
        slot = chip if sender else peer
        return remote(
            back.at[chunk, peer], prefix.at[chunk, slot], back_send.at[chunk, k], back_recv.at[chunk, slot], mate(k)
        )

    def hand(chunk):
        return remote(
            handed.at[chunk], received.at[chunk], hand_send.at[chunk], hand_recv.at[chunk], partner
        )

    first = side == 0
    mine_at = pl.ds(pl.multiple_of(side * half, half), half)

    def combine(chunk):
        swap_sides(chunk).wait_recv()
        a, b = own[chunk, mine_at, :CHUNK], other[chunk, :, :CHUNK]
        fa, fb = own[0, mine_at, CHUNK:], other[0, :, CHUNK:]
        late = across(jnp.where(first, fb, fa))
        both = late * jnp.where(first, a, b) + jnp.where(first, b, a)
        for p in range(chips):
            stage[chunk, p, :, :CHUNK] = both[p * piece : (p + 1) * piece]
            if chunk == 0:
                stage[chunk, p, :, CHUNK:] = (fa * fb)[p * piece : (p + 1) * piece]
        for k in range(1, chips):
            go(chunk, k, True).start()
        wide = CHUNK if chunk else CHUNK + LANES
        inbox[chunk, chip, :, :wide] = stage[chunk, chip, :, :wide]

    def give_all(chunk):
        for k in range(1, chips):
            give(chunk, k, True).start()
        prefix[chunk, chip] = back[chunk, chip]

    def scan_group(chunk):
        for k in range(1, chips):
            go(chunk, k, False).wait_recv()
        running = jnp.zeros((piece, CHUNK), jnp.float32)
        factor = jnp.ones((piece, LANES), jnp.float32)
        for m in range(chips):
            back[chunk, m] = running
            by = inbox[0, m, :, CHUNK:]
            if chunk == 0:
                spread[m] = factor
            running = across(by) * running + inbox[chunk, m, :, :CHUNK]
            if chunk == 0:
                factor = factor * by
        total[chunk, :, :CHUNK] = running
        if chunk == 0:
            total[chunk, :, CHUNK:] = factor
        for k in range(1, groups):

            @pl.when(group + k < groups)
            def _():
                up(chunk, k, group).start()

        @pl.when(group == 0)
        def _():
            give_all(chunk)

    def finish_groups(chunk):
        if groups == 1:
            return
        carried[...] = jnp.zeros((piece, CHUNK), jnp.float32)
        for g in range(groups - 1):

            @pl.when(g < group)
            def _():
                up(chunk, 1, g).wait_recv()
                by = earlier[0, g, :, CHUNK:]
                carried[...] = across(by) * carried[...] + earlier[chunk, g, :, :CHUNK]

        @pl.when(group > 0)
        def _():
            before = carried[...]
            for m in range(chips):
                back[chunk, m] += across(spread[m]) * before
            give_all(chunk)

    def pass_on(chunk):
        for k in range(1, chips):
            give(chunk, k, False).wait_recv()
        before = prefix[chunk].reshape(half, CHUNK)
        a, b = own[chunk, mine_at, :CHUNK], other[chunk, :, :CHUNK]
        fa, fb = own[0, mine_at, CHUNK:], other[0, :, CHUNK:]
        after = across(jnp.where(first, fa, fb)) * before + jnp.where(first, a, b)
        handed[chunk] = jnp.where(first, after, before)
        hand(chunk).start()
        out_ref[mine_at, chunk * CHUNK : (chunk + 1) * CHUNK] = jnp.where(first, before, after)

    def take(chunk):
        hand(chunk).wait_recv()
        at = pl.ds(pl.multiple_of((1 - side) * half, half), half)
        out_ref[at, chunk * CHUNK : (chunk + 1) * CHUNK] = received[chunk]

    for chunk in range(chunks):
        if chunk == 0:
            pl.semaphore_wait(barrier, len(peers))
        swap_sides(chunk).start()
    for chunk in range(chunks):
        combine(chunk)
    for chunk in range(chunks):
        scan_group(chunk)
    for chunk in range(chunks):
        finish_groups(chunk)
    for chunk in range(chunks):
        pass_on(chunk)
    for chunk in range(chunks):
        take(chunk)

    for chunk in range(chunks):
        swap_sides(chunk).wait_send()
        hand(chunk).wait_send()
        for k in range(1, chips):
            go(chunk, k, True).wait_send()
            give(chunk, k, True).wait_send()
        for k in range(1, groups):

            @pl.when(group + k < groups)
            def _():
                up(chunk, k, group).wait_send()


def before_own(n, running, fact):
    size = max(s for s in range(2, 2 * SLOTS // (2 * SUB) + 1, 2) if n % s == 0 and SLOTS % (s * SUB) == 0)
    groups, chips = n // size, size // 2
    half = SLOTS // 2
    piece, chunks = half // chips, COLS // CHUNK
    wide = CHUNK + LANES
    dma = pltpu.SemaphoreType.DMA
    f32 = lambda *shape: pltpu.VMEM(shape, jnp.float32)
    return pl.pallas_call(
        functools.partial(scan_kernel, n, size),
        out_shape=jax.ShapeDtypeStruct((SLOTS, COLS), jnp.float32),
        in_specs=[pl.BlockSpec(memory_space=pltpu.VMEM)] * 2,
        out_specs=pl.BlockSpec(memory_space=pltpu.VMEM),
        scratch_shapes=[
            f32(chunks, SLOTS, wide), f32(chunks, half, wide), f32(chunks, chips, piece, wide),
            f32(chunks, chips, piece, wide), f32(chunks, piece, wide), f32(chunks, groups, piece, wide),
            f32(piece, CHUNK), f32(chips, piece, LANES), f32(chunks, chips, piece, CHUNK),
            f32(chunks, chips, piece, CHUNK), f32(chunks, half, CHUNK), f32(chunks, half, CHUNK),
            dma((chunks,)), dma((chunks,)), dma((chunks,)), dma((chunks, chips)), dma((chunks, chips)),
            dma((chunks, groups)), dma((chunks, groups)), dma((chunks, chips)), dma((chunks, chips)),
            dma((chunks,)), dma((chunks,)),
        ],
        compiler_params=pltpu.CompilerParams(collective_id=0, has_side_effects=True, vmem_limit_bytes=16 * 2**20),
    )(running, fact)


def heat_kernel(running_ref, before_ref, fact_ref, out_hbm, out_ref, sem):
    windows = running_ref.shape[0]
    stores = []
    for channel in range(IMAGE_LAYERS):
        at = slice(channel * ROWS, (channel + 1) * ROWS)
        for window in range(windows):
            factor = jnp.concatenate([fact_ref[window, channel : channel + 1, :]] * (COLS // LANES), axis=1)
            out_ref[window, at] = factor * before_ref[at] + running_ref[window, at]
            stores.append(
                pltpu.make_async_copy(out_ref.at[window, at], out_hbm.at[window, at], sem.at[window, channel])
            )
            stores[-1].start()
    for store in stores:
        store.wait()


def heat(running, before, fact):
    windows = running.shape[0]
    return pl.pallas_call(
        heat_kernel,
        out_shape=jax.ShapeDtypeStruct(running.shape, jnp.float32),
        in_specs=[pl.BlockSpec(memory_space=pltpu.VMEM)] * 3,
        out_specs=pl.BlockSpec(memory_space=pltpu.HBM),
        scratch_shapes=[pltpu.VMEM(running.shape, jnp.float32), pltpu.SemaphoreType.DMA((windows, IMAGE_LAYERS))],
        compiler_params=pltpu.CompilerParams(vmem_limit_bytes=8 * 2**20),
    )(running, before, fact)


def local(n, point_rows, point_cols, point_chans, point_weights, decay):
    running, fact = binned(point_rows, point_cols, point_chans, point_weights, decay)
    before = before_own(n, running, fact)
    return heat(running, before, fact).reshape(-1, IMAGE_LAYERS, ROWS, COLS)


def solution(mesh):
    placed = (P("win", None),) * 5
    return jax.shard_map(
        functools.partial(local, mesh.shape["win"]),
        mesh=mesh, in_specs=placed, out_specs=P("win", None, None, None), check_vma=False,
    )
```

```python
import functools
import jax, jax.numpy as jnp
from jax import lax
from jax.experimental import pallas as pl
from jax.experimental.pallas import tpu as pltpu
from jax.sharding import PartitionSpec as P
IMAGE_LAYERS=4
SLOTS=128; ROWS=32; COLS=1024; PART=256; LANES=128; SUB=8
PARTS=2
UNROLL=8
STEP=2*UNROLL
def hot(index, on):
    spread = jnp.broadcast_to(index, (16, LANES)).astype(jnp.bfloat16)
    slots = lax.broadcasted_iota(jnp.int32, (16, LANES), 0).astype(jnp.float32).astype(jnp.bfloat16)
    off = jnp.zeros((16, LANES), jnp.bfloat16)
    return jnp.concatenate([jnp.where(spread == slots + jnp.bfloat16(16.0*g), on, off) for g in range(16)], axis=0)

def swap(x, bits):
    sub = lax.broadcasted_iota(jnp.int32, (SUB, LANES), 0)
    return jnp.take_along_axis(x, sub ^ bits, axis=0)

def exchange(xs, i, j):
    xs[i], xs[j] = jnp.minimum(xs[i], xs[j]), jnp.maximum(xs[i], xs[j])

def sort_rows(xs):
    n=len(xs); xs=list(xs)
    sub = lax.broadcasted_iota(jnp.int32, (SUB, LANES), 0)
    k=2
    while k<=n:
        for b in range(0,n,k):
            for t in range(k//2): exchange(xs,b+t,b+k-1-t)
        d=k//4
        while d:
            for i in range(n):
                if not i & d: exchange(xs,i,i+d)
            d//=2
        k*=2
    width=1
    while width<SUB:
        low = (sub & width)==0
        ys=[swap(x,2*width-1) for x in xs]
        xs=[jnp.where(low,jnp.minimum(xs[i],ys[n-1-i]),jnp.maximum(xs[i],ys[n-1-i])) for i in range(n)]
        d=width//2
        while d:
            low=(sub & d)==0
            xs=[jnp.where(low,jnp.minimum(x,y),jnp.maximum(x,y)) for x,y in ((x,swap(x,d)) for x in xs)]
            d//=2
        d=n//2
        while d:
            for i in range(n):
                if not i & d: exchange(xs,i,i+d)
            d//=2
        width*=2
    return xs

def splits(height):
    first, second = (height * cut // 8 // STEP * STEP for cut in (3, 5))
    return (0, first, second, height)


def right(where_, weigh, r):
    return jnp.concatenate([hot(where_[pl.ds(r+i,1),:],jnp.broadcast_to(weigh[pl.ds(r+i,1),:],(16,LANES)).astype(jnp.bfloat16)) for i in range(2)],axis=1)


def left(place, r, base):
    one=jnp.ones((16,LANES),jnp.bfloat16)
    return jnp.concatenate([hot(place[pl.ds(r+i,1),:]-base,one) for i in range(2)],axis=1)


def blocks(got, quarter):
    for block in range(8):
        index=4*quarter+block
        part,j,c=index//8,index//2%4,index%2
        yield slice(64*part+32*c,64*part+32*c+32),slice(256*j,256*j+256),2*part+c,got[32*block:32*block+32]


def kernel(rows_hbm, cols_hbm, chans_hbm, weights_hbm, decay_hbm, place, where_, weigh, spare, fact, rows, cols, chans, weights, decay, keys, odd, sem):
    copies=[pltpu.make_async_copy(a,b,sem.at[i]) for i,(a,b) in enumerate(((decay_hbm,decay),(weights_hbm,weights),(cols_hbm,cols),(chans_hbm,chans),(rows_hbm,rows)))]
    for copy in copies: copy.start()
    windows = spare.shape[0]
    spare[...] = jnp.zeros(spare.shape, jnp.float32)
    for copy in copies: copy.wait()
    pl.run_scoped(functools.partial(sort_points,rows,cols,chans,weights,decay,place,where_,weigh,spare,fact,keys,odd),
        *[pltpu.ACC(m)((256,256),jnp.float32) for m in range(2)])


def sort_points(rows, cols, chans, weights, decay, place, where_, weigh, spare, fact, keys, odd, *accs):
    windows = spare.shape[0]
    for channel in range(IMAGE_LAYERS):
        factor = jnp.float32(1.0)
        for w in range(windows):
            factor = factor * decay[w, channel]
            fact[w, channel : channel + 1, :] = jnp.full((1, LANES), factor, jnp.float32)
            at = IMAGE_LAYERS + channel
            fact[w, at : at + 1, :] = jnp.full((1, LANES), decay[w, channel], jnp.float32)
    total = rows.shape[0]; height = total//windows
    _, first, second, _ = splits(height)
    for v in range(total//16):
        at=pl.ds(16*v,16)
        c=cols[at,:]; k=chans[at,:]
        w=(weights[at,:].astype(jnp.float32)*512.0).astype(jnp.int32)
        lidx=((k>>1)<<8)|((c>>8)<<6)|((k&1)<<5)|rows[at,:]
        keys[at,:]=(lidx<<20)|((c&255)<<12)|w
    n=height//SUB
    ranks=lax.broadcasted_iota(jnp.int32,(SUB,LANES),0)*n
    bounds=[]
    for w in range(windows):
        xs=[keys[pl.ds(w+windows*SUB*v,SUB,stride=windows),:] for v in range(n)]
        xs=sort_rows(xs)
        least=jnp.full((SUB,LANES),height,jnp.int32); most=jnp.full((SUB,LANES),-1,jnp.int32)
        for v in range(n):
            x=xs[v]
            index=x>>20
            rank=ranks+v
            base=jnp.where(rank<first,0,jnp.where(rank<second,128,256))
            out_of=(index<base)|(index>=base+256)
            least=jnp.minimum(least,jnp.where(out_of,rank,height))
            most=jnp.maximum(most,jnp.where(out_of,rank,-1))
            at=pl.ds(w*height+v,SUB,stride=n)
            index=index.astype(jnp.float32)
            place[at,:]=index
            odd[at,:]=jnp.where(out_of,index,-1000.0)
            where_[at,:]=((x>>12)&255).astype(jnp.float32)
            weigh[at,:]=(x&4095).astype(jnp.float32)*(1.0/512.0)
        bounds.append((jnp.min(least),jnp.max(most)))
    rest=slice(total,place.shape[0]); size=(place.shape[0]-total,LANES)
    place[rest,:]=jnp.full(size,-1000.0,jnp.float32)
    where_[rest,:]=jnp.zeros(size,jnp.float32)
    weigh[rest,:]=jnp.zeros(size,jnp.float32)
    for w in range(windows):
        least,most=bounds[w]

        @pl.when(most>=least)
        def _():
            begin=(least>>2)<<2
            for quarter in (0,2):
                for m in range(2): pltpu.matmul_pop(accs[m])

                def body(i,c):
                    for m in range(2):
                        r=w*height+begin+4*i+2*m
                        pltpu.matmul_push_rhs(right(where_,weigh,r),staging_register=0,mxu_index=m,transpose=True)
                        pltpu.matmul_acc_lhs(accs[m],left(odd,r,128.0*quarter),load_staged_rhs=0)
                    return c
                lax.fori_loop(0,(most-begin)//4+1,body,0)
                for at,across_,_,piece in blocks(pltpu.matmul_pop(accs[0])+pltpu.matmul_pop(accs[1]),quarter):
                    spare[w,at,across_]=piece


def view(x):
    windows,count=x.shape
    return x.reshape(windows,count//LANES,LANES).transpose(1,0,2).reshape(windows*count//LANES,LANES)
def binned(r,c,k,w,d):
    windows,count=r.shape
    height=count//LANES
    tall=windows*height
    points=jax.ShapeDtypeStruct((tall+SUB,LANES),jnp.float32)
    return pl.pallas_call(
        kernel,
        out_shape=(
            points, points, points,
            jax.ShapeDtypeStruct((windows, SLOTS, COLS), jnp.float32),
            jax.ShapeDtypeStruct((windows, SUB, LANES), jnp.float32),
        ),
        in_specs=[pl.BlockSpec(memory_space=pltpu.HBM)] * 5,
        out_specs=[pl.BlockSpec(memory_space=pltpu.VMEM)] * 5,
        scratch_shapes=[pltpu.VMEM((tall, LANES), jnp.int32)] * 3
        + [pltpu.VMEM((tall, LANES), jnp.bfloat16), pltpu.SMEM(d.shape, jnp.float32)]
        + [pltpu.VMEM((tall, LANES), jnp.int32), pltpu.VMEM((tall, LANES), jnp.float32)]
        + [pltpu.SemaphoreType.DMA((5,))],
        compiler_params=pltpu.CompilerParams(vmem_limit_bytes=16 * 2**20),
    )(*(pltpu.with_memory_space_constraint(x, pltpu.HBM) for x in (*map(view, (r, c, k, w)), d)))


MESH = pl.DeviceIdType.MESH
CHUNK = 512


def across(tile):
    return jnp.concatenate([tile] * (CHUNK // LANES), axis=1)


def bin_points(place, where_, weigh, spare, fact, running, ahead, *accs):
    windows = running.shape[0]
    height = (place.shape[0] - SUB) // windows
    cuts = splits(height)
    for acc in accs:
        running[0, :, :PART] = pltpu.matmul_pop(acc)[:SLOTS]

    def prepare(m, staging, r, base):
        pltpu.matmul_push_rhs(right(where_, weigh, r), staging_register=staging, mxu_index=m, transpose=True)
        ahead[m] = left(place, r, base)

    def multiply(targets, begin, trips, base, then):
        def body(i, carry):
            for u in range(UNROLL):
                m, s = u % 2, u // 2 % 2
                r = begin + i * STEP + 2 * u
                pltpu.matmul_push_rhs(
                    right(where_, weigh, r + 4), staging_register=1 - s, mxu_index=m, transpose=True
                )
                pltpu.matmul_acc_lhs(targets[m], ahead[m] if u < 2 else left(place, r, base), load_staged_rhs=s)
                if u >= UNROLL - 2:
                    ahead[m] = left(place, r + 4, jnp.where(i == trips - 1, then, base))
            return carry

        lax.fori_loop(0, trips, body, 0)

    def gather(w, phase, add):
        got = pltpu.matmul_pop(accs[2 * phase]) + pltpu.matmul_pop(accs[2 * phase + 1])
        for at, across_, channel, piece in blocks(got, phase):
            if add:
                running[w, at, across_] += piece
                continue
            piece = piece + spare[w, at, across_]
            if w:
                row = fact[w, IMAGE_LAYERS + channel : IMAGE_LAYERS + channel + 1, :]
                piece = jnp.concatenate([row] * (PART // LANES), axis=1) * running[w - 1, at, across_] + piece
            running[w, at, across_] = piece

    for m in range(2):
        prepare(m, 0, 2 * m, jnp.float32(0.0))
    for w in range(windows):
        for p in range(3):
            trips = (cuts[p + 1] - cuts[p]) // STEP
            multiply(
                accs[2 * p : 2 * p + 2], w * height + cuts[p], trips,
                jnp.float32(128.0 * p), jnp.float32(128.0 * ((p + 1) % 3)),
            )
        for p in (0, 2, 1):
            gather(w, p, p == 1)
    for m in range(2):
        pltpu.matmul_acc_lhs(accs[m], jnp.zeros((256, 256), jnp.bfloat16), load_staged_rhs=0)
    running[0, :1, :PART] += (pltpu.matmul_pop(accs[0]) + pltpu.matmul_pop(accs[1]))[:1]


def scan_kernel(
    n, size, place, where_, weigh, spare, fact_ref, running_hbm, out_ref,
    ahead, own, other, stage, inbox, total, earlier, carried, spread, back, prefix, handed, received,
    load_sem, swap_send, swap_recv, go_send, go_recv, up_send, up_recv, back_send, back_recv, hand_send, hand_recv,
):
    windows = running_hbm.shape[0]
    groups, chips = n // size, size // 2
    half = SLOTS // 2
    piece = half // chips
    chunks = COLS // CHUNK
    me = lax.axis_index("win")
    group, member = lax.div(me, size), lax.rem(me, size)
    chip, side = lax.div(member, 2), lax.rem(member, 2)
    partner = me + 1 - 2 * side
    mate = lambda k: group * size + 2 * lax.rem(chip + k, chips) + side
    counter = lambda k: lax.rem(me + k * size, n)

    barrier = pltpu.get_barrier_semaphore()
    peers = [partner] + [mate(k) for k in range(1, chips)] + [counter(k) for k in range(1, groups)]
    for peer in peers:
        pl.semaphore_signal(barrier, inc=1, device_id=(peer,), device_id_type=MESH)
    pl.run_scoped(
        functools.partial(bin_points, place, where_, weigh, spare, fact_ref, running_hbm, ahead),
        *[pltpu.ACC(m)((256, 256), jnp.float32) for _ in range(3) for m in range(2)],
    )
    for c in range(chunks):
        own[c, :, :CHUNK] = running_hbm[windows - 1, :, c * CHUNK : (c + 1) * CHUNK]
    for channel in range(IMAGE_LAYERS):
        factor = fact_ref[windows - 1, channel : channel + 1, :]
        own[0, channel * ROWS : (channel + 1) * ROWS, CHUNK:] = jnp.broadcast_to(factor, (ROWS, LANES))

    def sent(ref, chunk):
        return ref if chunk == 0 else ref.at[:, pl.ds(0, CHUNK)]

    def remote(src, dst, send, recv, device):
        return pltpu.make_async_remote_copy(
            src_ref=src, dst_ref=dst, send_sem=send, recv_sem=recv, device_id=(device,), device_id_type=MESH
        )

    def swap_sides(chunk):
        away = own.at[chunk, pl.ds(pl.multiple_of((1 - side) * half, half), half)]
        return remote(
            sent(away, chunk), sent(other.at[chunk], chunk), swap_send.at[chunk], swap_recv.at[chunk], partner
        )

    def go(chunk, k, sender):
        peer = lax.rem(chip + k, chips)
        slot = chip if sender else peer
        return remote(
            sent(stage.at[chunk, peer], chunk), sent(inbox.at[chunk, slot], chunk),
            go_send.at[chunk, k], go_recv.at[chunk, slot], mate(k),
        )

    def up(chunk, k, slot):
        return remote(
            sent(total.at[chunk], chunk), sent(earlier.at[chunk, slot], chunk),
            up_send.at[chunk, k], up_recv.at[chunk, slot], counter(k),
        )

    def give(chunk, k, sender):
        peer = lax.rem(chip + k, chips)
        slot = chip if sender else peer
        return remote(
            back.at[chunk, peer], prefix.at[chunk, slot], back_send.at[chunk, k], back_recv.at[chunk, slot], mate(k)
        )

    def hand(chunk):
        return remote(
            handed.at[chunk], received.at[chunk], hand_send.at[chunk], hand_recv.at[chunk], partner
        )

    first = side == 0
    mine_at = pl.ds(pl.multiple_of(side * half, half), half)

    def combine(chunk):
        swap_sides(chunk).wait_recv()
        a, b = own[chunk, mine_at, :CHUNK], other[chunk, :, :CHUNK]
        fa, fb = own[0, mine_at, CHUNK:], other[0, :, CHUNK:]
        late = across(jnp.where(first, fb, fa))
        both = late * jnp.where(first, a, b) + jnp.where(first, b, a)
        for p in range(chips):
            stage[chunk, p, :, :CHUNK] = both[p * piece : (p + 1) * piece]
            if chunk == 0:
                stage[chunk, p, :, CHUNK:] = (fa * fb)[p * piece : (p + 1) * piece]
        for k in range(1, chips):
            go(chunk, k, True).start()
        wide = CHUNK if chunk else CHUNK + LANES
        inbox[chunk, chip, :, :wide] = stage[chunk, chip, :, :wide]

    def give_all(chunk):
        for k in range(1, chips):
            give(chunk, k, True).start()
        prefix[chunk, chip] = back[chunk, chip]

    def scan_group(chunk):
        for k in range(1, chips):
            go(chunk, k, False).wait_recv()
        running = jnp.zeros((piece, CHUNK), jnp.float32)
        factor = jnp.ones((piece, LANES), jnp.float32)
        for m in range(chips):
            back[chunk, m] = running
            by = inbox[0, m, :, CHUNK:]
            if chunk == 0:
                spread[m] = factor
            running = across(by) * running + inbox[chunk, m, :, :CHUNK]
            if chunk == 0:
                factor = factor * by
        total[chunk, :, :CHUNK] = running
        if chunk == 0:
            total[chunk, :, CHUNK:] = factor
        for k in range(1, groups):

            @pl.when(group + k < groups)
            def _():
                up(chunk, k, group).start()

        @pl.when(group == 0)
        def _():
            give_all(chunk)

    def finish_groups(chunk):
        if groups == 1:
            return
        carried[...] = jnp.zeros((piece, CHUNK), jnp.float32)
        for g in range(groups - 1):

            @pl.when(g < group)
            def _():
                up(chunk, 1, g).wait_recv()
                by = earlier[0, g, :, CHUNK:]
                carried[...] = across(by) * carried[...] + earlier[chunk, g, :, :CHUNK]

        @pl.when(group > 0)
        def _():
            before = carried[...]
            for m in range(chips):
                back[chunk, m] += across(spread[m]) * before
            give_all(chunk)

    def pass_on(chunk):
        for k in range(1, chips):
            give(chunk, k, False).wait_recv()
        before = prefix[chunk].reshape(half, CHUNK)
        a, b = own[chunk, mine_at, :CHUNK], other[chunk, :, :CHUNK]
        fa, fb = own[0, mine_at, CHUNK:], other[0, :, CHUNK:]
        after = across(jnp.where(first, fa, fb)) * before + jnp.where(first, a, b)
        handed[chunk] = jnp.where(first, after, before)
        hand(chunk).start()
        out_ref[mine_at, chunk * CHUNK : (chunk + 1) * CHUNK] = jnp.where(first, before, after)

    def take(chunk):
        hand(chunk).wait_recv()
        at = pl.ds(pl.multiple_of((1 - side) * half, half), half)
        out_ref[at, chunk * CHUNK : (chunk + 1) * CHUNK] = received[chunk]

    for chunk in range(chunks):
        if chunk == 0:
            pl.semaphore_wait(barrier, len(peers))
        swap_sides(chunk).start()
    for chunk in range(chunks):
        combine(chunk)
    for chunk in range(chunks):
        scan_group(chunk)
    for chunk in range(chunks):
        finish_groups(chunk)
    for chunk in range(chunks):
        pass_on(chunk)
    for chunk in range(chunks):
        take(chunk)

    for chunk in range(chunks):
        swap_sides(chunk).wait_send()
        hand(chunk).wait_send()
        for k in range(1, chips):
            go(chunk, k, True).wait_send()
            give(chunk, k, True).wait_send()
        for k in range(1, groups):

            @pl.when(group + k < groups)
            def _():
                up(chunk, k, group).wait_send()


def before_own(n, place, where_, weigh, spare, fact):
    windows = spare.shape[0]
    size = max(s for s in range(2, 2 * SLOTS // (2 * SUB) + 1, 2) if n % s == 0 and SLOTS % (s * SUB) == 0)
    groups, chips = n // size, size // 2
    half = SLOTS // 2
    piece, chunks = half // chips, COLS // CHUNK
    wide = CHUNK + LANES
    dma = pltpu.SemaphoreType.DMA
    f32 = lambda *shape: pltpu.VMEM(shape, jnp.float32)
    return pl.pallas_call(
        functools.partial(scan_kernel, n, size),
        out_shape=(
            jax.ShapeDtypeStruct((windows, SLOTS, COLS), jnp.float32),
            jax.ShapeDtypeStruct((SLOTS, COLS), jnp.float32),
        ),
        in_specs=[pl.BlockSpec(memory_space=pltpu.VMEM)] * 5,
        out_specs=[pl.BlockSpec(memory_space=pltpu.VMEM)] * 2,
        scratch_shapes=[
            pltpu.VMEM((2, 256, 256), jnp.bfloat16),
            f32(chunks, SLOTS, wide), f32(chunks, half, wide), f32(chunks, chips, piece, wide),
            f32(chunks, chips, piece, wide), f32(chunks, piece, wide), f32(chunks, groups, piece, wide),
            f32(piece, CHUNK), f32(chips, piece, LANES), f32(chunks, chips, piece, CHUNK),
            f32(chunks, chips, piece, CHUNK), f32(chunks, half, CHUNK), f32(chunks, half, CHUNK),
            dma((chunks,)), dma((chunks,)), dma((chunks,)), dma((chunks, chips)), dma((chunks, chips)),
            dma((chunks, groups)), dma((chunks, groups)), dma((chunks, chips)), dma((chunks, chips)),
            dma((chunks,)), dma((chunks,)),
        ],
        compiler_params=pltpu.CompilerParams(collective_id=0, has_side_effects=True, vmem_limit_bytes=16 * 2**20),
    )(place, where_, weigh, spare, fact)


def heat_kernel(running_ref, before_ref, fact_ref, out_hbm, out_ref, sem):
    windows = running_ref.shape[0]
    stores = []
    for channel in range(IMAGE_LAYERS):
        at = slice(channel * ROWS, (channel + 1) * ROWS)
        for window in range(windows):
            factor = jnp.concatenate([fact_ref[window, channel : channel + 1, :]] * (COLS // LANES), axis=1)
            out_ref[window, at] = factor * before_ref[at] + running_ref[window, at]
            stores.append(
                pltpu.make_async_copy(out_ref.at[window, at], out_hbm.at[window, at], sem.at[window, channel])
            )
            stores[-1].start()
    for store in stores:
        store.wait()


def heat(running, before, fact):
    windows = running.shape[0]
    return pl.pallas_call(
        heat_kernel,
        out_shape=jax.ShapeDtypeStruct(running.shape, jnp.float32),
        in_specs=[pl.BlockSpec(memory_space=pltpu.VMEM)] * 3,
        out_specs=pl.BlockSpec(memory_space=pltpu.HBM),
        scratch_shapes=[pltpu.VMEM(running.shape, jnp.float32), pltpu.SemaphoreType.DMA((windows, IMAGE_LAYERS))],
        compiler_params=pltpu.CompilerParams(vmem_limit_bytes=8 * 2**20),
    )(running, before, fact)


def local(n, point_rows, point_cols, point_chans, point_weights, decay):
    *points, fact = binned(point_rows, point_cols, point_chans, point_weights, decay)
    running, before = before_own(n, *points, fact)
    return heat(running, before, fact).reshape(-1, IMAGE_LAYERS, ROWS, COLS)


def solution(mesh):
    placed = (P("win", None),) * 5
    return jax.shard_map(
        functools.partial(local, mesh.shape["win"]),
        mesh=mesh, in_specs=placed, out_specs=P("win", None, None, None), check_vma=False,
    )
```

```python
import functools
import jax, jax.numpy as jnp
from jax import lax
from jax.experimental import pallas as pl
from jax.experimental.pallas import tpu as pltpu
from jax.sharding import PartitionSpec as P
IMAGE_LAYERS=4
SLOTS=128; ROWS=32; COLS=1024; PART=256; LANES=128; SUB=8
PARTS=2
UNROLL=8
STEP=2*UNROLL
def hot(index, on):
    spread = jnp.broadcast_to(index, (16, LANES)).astype(jnp.bfloat16)
    slots = lax.broadcasted_iota(jnp.int32, (16, LANES), 0).astype(jnp.float32).astype(jnp.bfloat16)
    off = jnp.zeros((16, LANES), jnp.bfloat16)
    return jnp.concatenate([jnp.where(spread == slots + jnp.bfloat16(16.0*g), on, off) for g in range(16)], axis=0)

def swap(x, bits):
    sub = lax.broadcasted_iota(jnp.int32, (SUB, LANES), 0)
    return jnp.take_along_axis(x, sub ^ bits, axis=0)

def exchange(xs, i, j):
    xs[i], xs[j] = jnp.minimum(xs[i], xs[j]), jnp.maximum(xs[i], xs[j])

def sort_rows(xs):
    n=len(xs); xs=list(xs)
    sub = lax.broadcasted_iota(jnp.int32, (SUB, LANES), 0)
    k=2
    while k<=n:
        for b in range(0,n,k):
            for t in range(k//2): exchange(xs,b+t,b+k-1-t)
        d=k//4
        while d:
            for i in range(n):
                if not i & d: exchange(xs,i,i+d)
            d//=2
        k*=2
    width=1
    while width<SUB:
        low = (sub & width)==0
        ys=[swap(x,2*width-1) for x in xs]
        xs=[jnp.where(low,jnp.minimum(xs[i],ys[n-1-i]),jnp.maximum(xs[i],ys[n-1-i])) for i in range(n)]
        d=width//2
        while d:
            low=(sub & d)==0
            xs=[jnp.where(low,jnp.minimum(x,y),jnp.maximum(x,y)) for x,y in ((x,swap(x,d)) for x in xs)]
            d//=2
        d=n//2
        while d:
            for i in range(n):
                if not i & d: exchange(xs,i,i+d)
            d//=2
        width*=2
    return xs

def splits(height):
    first, second = (height * cut // 8 // STEP * STEP for cut in (3, 5))
    return (0, first, second, height)


def right(where_, weigh, r):
    return jnp.concatenate([hot(where_[pl.ds(r+i,1),:],jnp.broadcast_to(weigh[pl.ds(r+i,1),:],(16,LANES)).astype(jnp.bfloat16)) for i in range(2)],axis=1)


def left(place, r, base):
    one=jnp.ones((16,LANES),jnp.bfloat16)
    return jnp.concatenate([hot(place[pl.ds(r+i,1),:]-base,one) for i in range(2)],axis=1)


def blocks(got, quarter):
    for block in range(8):
        index=4*quarter+block
        part,j,c=index//8,index//2%4,index%2
        yield slice(64*part+32*c,64*part+32*c+32),slice(256*j,256*j+256),2*part+c,got[32*block:32*block+32]


def kernel(rows_hbm, cols_hbm, chans_hbm, weights_hbm, decay_hbm, place, where_, weigh, spare, fact, rows, cols, chans, weights, decay, keys, odd, sem):
    copies=[pltpu.make_async_copy(a,b,sem.at[i]) for i,(a,b) in enumerate(((decay_hbm,decay),(weights_hbm,weights),(cols_hbm,cols),(chans_hbm,chans),(rows_hbm,rows)))]
    for copy in copies: copy.start()
    windows = spare.shape[0]
    spare[...] = jnp.zeros(spare.shape, jnp.float32)
    for copy in copies: copy.wait()
    pl.run_scoped(functools.partial(sort_points,rows,cols,chans,weights,decay,place,where_,weigh,spare,fact,keys,odd),
        *[pltpu.ACC(m)((256,256),jnp.float32) for m in range(2)])


def sort_points(rows, cols, chans, weights, decay, place, where_, weigh, spare, fact, keys, odd, *accs):
    windows = spare.shape[0]
    for channel in range(IMAGE_LAYERS):
        factor = jnp.float32(1.0)
        for w in range(windows):
            factor = factor * decay[w, channel]
            fact[w, channel : channel + 1, :] = jnp.full((1, LANES), factor, jnp.float32)
            at = IMAGE_LAYERS + channel
            fact[w, at : at + 1, :] = jnp.full((1, LANES), decay[w, channel], jnp.float32)
    total = rows.shape[0]; height = total//windows
    _, first, second, _ = splits(height)
    for v in range(total//16):
        at=pl.ds(16*v,16)
        c=cols[at,:]; k=chans[at,:]
        w=(weights[at,:].astype(jnp.float32)*512.0).astype(jnp.int32)
        lidx=((k>>1)<<8)|((c>>8)<<6)|((k&1)<<5)|rows[at,:]
        keys[at,:]=(lidx<<20)|((c&255)<<12)|w
    n=height//SUB
    ranks=lax.broadcasted_iota(jnp.int32,(SUB,LANES),0)*n
    bounds=[]
    for w in range(windows):
        xs=[keys[pl.ds(w+windows*SUB*v,SUB,stride=windows),:] for v in range(n)]
        xs=sort_rows(xs)
        least=jnp.full((SUB,LANES),height,jnp.int32); most=jnp.full((SUB,LANES),-1,jnp.int32)
        for v in range(n):
            x=xs[v]
            index=x>>20
            rank=ranks+v
            base=jnp.where(rank<first,0,jnp.where(rank<second,128,256))
            out_of=(index<base)|(index>=base+256)
            least=jnp.minimum(least,jnp.where(out_of,rank,height))
            most=jnp.maximum(most,jnp.where(out_of,rank,-1))
            at=pl.ds(w*height+v,SUB,stride=n)
            index=index.astype(jnp.float32)
            place[at,:]=index
            odd[at,:]=jnp.where(out_of,index,-1000.0)
            where_[at,:]=((x>>12)&255).astype(jnp.float32)
            weigh[at,:]=(x&4095).astype(jnp.float32)*(1.0/512.0)
        bounds.append((jnp.min(least),jnp.max(most)))
    rest=slice(total,place.shape[0]); size=(place.shape[0]-total,LANES)
    place[rest,:]=jnp.full(size,-1000.0,jnp.float32)
    where_[rest,:]=jnp.zeros(size,jnp.float32)
    weigh[rest,:]=jnp.zeros(size,jnp.float32)
    for w in range(windows):
        least,most=bounds[w]

        @pl.when(most>=least)
        def _():
            begin=(least>>2)<<2
            for quarter in (0,2):
                for m in range(2): pltpu.matmul_pop(accs[m])

                def body(i,c):
                    for m in range(2):
                        r=w*height+begin+4*i+2*m
                        pltpu.matmul_push_rhs(right(where_,weigh,r),staging_register=0,mxu_index=m,transpose=True)
                        pltpu.matmul_acc_lhs(accs[m],left(odd,r,128.0*quarter),load_staged_rhs=0)
                    return c
                lax.fori_loop(0,(most-begin)//4+1,body,0)
                for at,across_,_,piece in blocks(pltpu.matmul_pop(accs[0])+pltpu.matmul_pop(accs[1]),quarter):
                    spare[w,at,across_]=piece


def view(x):
    windows,count=x.shape
    return x.reshape(windows,count//LANES,LANES).transpose(1,0,2).reshape(windows*count//LANES,LANES)
def binned(r,c,k,w,d):
    windows,count=r.shape
    height=count//LANES
    tall=windows*height
    points=jax.ShapeDtypeStruct((tall+SUB,LANES),jnp.float32)
    return pl.pallas_call(
        kernel,
        out_shape=(
            points, points, points,
            jax.ShapeDtypeStruct((windows, SLOTS, COLS), jnp.float32),
            jax.ShapeDtypeStruct((windows, SUB, LANES), jnp.float32),
        ),
        in_specs=[pl.BlockSpec(memory_space=pltpu.HBM)] * 5,
        out_specs=[pl.BlockSpec(memory_space=pltpu.VMEM)] * 5,
        scratch_shapes=[pltpu.VMEM((tall, LANES), jnp.int32)] * 3
        + [pltpu.VMEM((tall, LANES), jnp.bfloat16), pltpu.SMEM(d.shape, jnp.float32)]
        + [pltpu.VMEM((tall, LANES), jnp.int32), pltpu.VMEM((tall, LANES), jnp.float32)]
        + [pltpu.SemaphoreType.DMA((5,))],
        compiler_params=pltpu.CompilerParams(vmem_limit_bytes=16 * 2**20),
    )(*(pltpu.with_memory_space_constraint(x, pltpu.HBM) for x in (*map(view, (r, c, k, w)), d)))


MESH = pl.DeviceIdType.MESH
CHUNK = 512


def across(tile):
    return jnp.concatenate([tile] * (CHUNK // LANES), axis=1)


class Bins:
    def __init__(self, place, where_, weigh, spare, fact, running, ahead, own, unused, accs):
        self.refs = place, where_, weigh
        self.spare, self.fact, self.running, self.ahead, self.own, self.unused = spare, fact, running, ahead, own, unused
        self.accs = accs
        self.windows = running.shape[0]
        self.height = (place.shape[0] - SUB) // self.windows
        self.cuts = splits(self.height)
        self.order = [(w, p) for p in range(3) for w in range(self.windows)]
        for acc in accs:
            unused[:, :PART] = pltpu.matmul_pop(acc)[: unused.shape[0]]
        for m in range(2):
            self.push(m, 0, self.start(0) + 2 * m)
            ahead[m] = left(place, self.start(0) + 2 * m, jnp.float32(0.0))

    def start(self, k):
        w, p = self.order[k % len(self.order)]
        return w * self.height + self.cuts[p]

    def push(self, m, staging, r):
        pltpu.matmul_push_rhs(right(*self.refs[1:], r), staging_register=staging, mxu_index=m, transpose=True)

    def region(self, w, p):
        at = 2 * (w + self.windows * (p % 2))
        return self.accs[at : at + 2]

    def multiply(self, w, p):
        k = self.order.index((w, p))
        trips = (self.cuts[p + 1] - self.cuts[p]) // STEP
        base, then = 128.0 * p, 128.0 * self.order[(k + 1) % len(self.order)][1]

        def body(i, carry):
            for u in range(UNROLL):
                m, s = u % 2, u // 2 % 2
                r = self.start(k) + i * STEP + 2 * u
                ending = u >= UNROLL - 2
                later = jnp.where(i == trips - 1, self.start(k + 1) + 2 * m, r + 4) if ending else r + 4
                self.push(m, 1 - s, later)
                hot_left = self.ahead[m] if u < 2 else left(self.refs[0], r, base)
                pltpu.matmul_acc_lhs(self.region(w, p)[m], hot_left, load_staged_rhs=s)
                if ending:
                    self.ahead[m] = left(self.refs[0], later, jnp.where(i == trips - 1, then, base))
            return carry

        lax.fori_loop(0, trips, body, 0)

    def pop(self, w, p):
        first, second = self.region(w, p)
        got = pltpu.matmul_pop(first) + pltpu.matmul_pop(second)
        return [got[32 * b : 32 * b + 32] for b in range(8)]

    def settle(self, part, w, pieces):
        for b, piece in enumerate(pieces):
            j, c = b // 2, b % 2
            channel = 2 * part + c
            at, wide = slice(ROWS * channel, ROWS * channel + ROWS), slice(PART * j, PART * j + PART)
            piece = piece + self.spare[w, at, wide]
            if w:
                row = self.fact[w, IMAGE_LAYERS + channel : IMAGE_LAYERS + channel + 1, :]
                piece = jnp.concatenate([row] * (PART // LANES), axis=1) * self.running[w - 1, at, wide] + piece
            self.running[w, at, wide] = piece
            if w == self.windows - 1:
                per = CHUNK // PART
                down = c * (COLS // CHUNK) * ROWS + j // per * ROWS
                self.own[part, down : down + ROWS, j % per * PART : (j % per + 1) * PART] = piece

    def settle_first(self):
        for w in range(self.windows):
            outer, inner = self.pop(w, 0), self.pop(w, 1)
            self.settle(0, w, outer[:4] + [x + y for x, y in zip(outer[4:], inner[:4])])
            for b, piece in enumerate(inner[4:]):
                at = (2 + b % 2) * ROWS
                self.running[w, at : at + ROWS, b // 2 * PART : (b // 2 + 1) * PART] = piece

    def settle_second(self):
        for w in range(self.windows):
            pieces = self.pop(w, 2)
            for b in range(4):
                at = (2 + b % 2) * ROWS
                pieces[b] = pieces[b] + self.running[w, at : at + ROWS, b // 2 * PART : (b // 2 + 1) * PART]
            self.settle(1, w, pieces)

    def close(self):
        for m in range(2):
            pltpu.matmul_acc_lhs(self.accs[m], jnp.zeros((256, 256), jnp.bfloat16), load_staged_rhs=0)
            self.unused[:, :PART] = pltpu.matmul_pop(self.accs[m])[: self.unused.shape[0]]


def scan_kernel(n, size, *refs):
    windows = refs[5].shape[0]
    pl.run_scoped(
        lambda *accs: scan(n, size, accs, *refs),
        *[pltpu.ACC(m)((256, PART), jnp.float32) for _ in range(2 * windows) for m in range(2)],
    )


def scan(
    n, size, accs, place, where_, weigh, spare, fact_ref, running_ref, out_ref,
    ahead, own, other, stage, inbox, total, earlier, carried, spread, back, prefix, handed, received,
    swap_send, swap_recv, go_send, go_recv, up_send, up_recv, back_send, back_recv, hand_send, hand_recv,
):
    windows = running_ref.shape[0]
    groups, chips = n // size, size // 2
    half = COLS // CHUNK * ROWS
    piece = half // chips
    chunks = IMAGE_LAYERS // 2
    me = lax.axis_index("win")
    group, member = lax.div(me, size), lax.rem(me, size)
    chip, side = lax.div(member, 2), lax.rem(member, 2)
    partner = me + 1 - 2 * side
    mate = lambda k: group * size + 2 * lax.rem(chip + k, chips) + side
    counter = lambda k: lax.rem(me + k * size, n)

    barrier = pltpu.get_barrier_semaphore()
    peers = [partner] + [mate(k) for k in range(1, chips)] + [counter(k) for k in range(1, groups)]
    for peer in peers:
        pl.semaphore_signal(barrier, inc=1, device_id=(peer,), device_id_type=MESH)
    for channel in range(IMAGE_LAYERS):
        factor = fact_ref[windows - 1, channel : channel + 1, :]
        down = channel % 2 * half
        own[channel // 2, down : down + half, CHUNK:] = jnp.broadcast_to(factor, (half, LANES))
    bins = Bins(place, where_, weigh, spare, fact_ref, running_ref, ahead, own, carried, accs)

    def remote(src, dst, send, recv, device):
        return pltpu.make_async_remote_copy(
            src_ref=src, dst_ref=dst, send_sem=send, recv_sem=recv, device_id=(device,), device_id_type=MESH
        )

    def swap_sides(chunk):
        away = own.at[chunk, pl.ds(pl.multiple_of((1 - side) * half, half), half)]
        return remote(
            away, other.at[chunk], swap_send.at[chunk], swap_recv.at[chunk], partner
        )

    def go(chunk, k, sender):
        peer = lax.rem(chip + k, chips)
        slot = chip if sender else peer
        return remote(
            stage.at[chunk, peer], inbox.at[chunk, slot],
            go_send.at[chunk, k], go_recv.at[chunk, slot], mate(k),
        )

    def up(chunk, k, slot):
        return remote(
            total.at[chunk], earlier.at[chunk, slot],
            up_send.at[chunk, k], up_recv.at[chunk, slot], counter(k),
        )

    def give(chunk, k, sender):
        peer = lax.rem(chip + k, chips)
        slot = chip if sender else peer
        return remote(
            back.at[chunk, peer], prefix.at[chunk, slot], back_send.at[chunk, k], back_recv.at[chunk, slot], mate(k)
        )

    def hand(chunk):
        return remote(
            handed.at[chunk], received.at[chunk], hand_send.at[chunk], hand_recv.at[chunk], partner
        )

    first = side == 0
    mine_at = pl.ds(pl.multiple_of(side * half, half), half)

    def combine(chunk):
        swap_sides(chunk).wait_recv()
        a, b = own[chunk, mine_at, :CHUNK], other[chunk, :, :CHUNK]
        fa, fb = own[chunk, mine_at, CHUNK:], other[chunk, :, CHUNK:]
        late = across(jnp.where(first, fb, fa))
        both = late * jnp.where(first, a, b) + jnp.where(first, b, a)
        for p in range(chips):
            stage[chunk, p, :, :CHUNK] = both[p * piece : (p + 1) * piece]
            stage[chunk, p, :, CHUNK:] = (fa * fb)[p * piece : (p + 1) * piece]
        for k in range(1, chips):
            go(chunk, k, True).start()
        inbox[chunk, chip] = stage[chunk, chip]

    def give_all(chunk):
        for k in range(1, chips):
            give(chunk, k, True).start()
        prefix[chunk, chip] = back[chunk, chip]

    def scan_group(chunk):
        for k in range(1, chips):
            go(chunk, k, False).wait_recv()
        running = jnp.zeros((piece, CHUNK), jnp.float32)
        factor = jnp.ones((piece, LANES), jnp.float32)
        for m in range(chips):
            back[chunk, m] = running
            by = inbox[chunk, m, :, CHUNK:]
            spread[chunk, m] = factor
            running = across(by) * running + inbox[chunk, m, :, :CHUNK]
            factor = factor * by
        total[chunk, :, :CHUNK] = running
        total[chunk, :, CHUNK:] = factor
        for k in range(1, groups):

            @pl.when(group + k < groups)
            def _():
                up(chunk, k, group).start()

        @pl.when(group == 0)
        def _():
            give_all(chunk)

    def finish_groups(chunk):
        if groups == 1:
            return
        carried[...] = jnp.zeros((piece, CHUNK), jnp.float32)
        for g in range(groups - 1):

            @pl.when(g < group)
            def _():
                up(chunk, 1, g).wait_recv()
                by = earlier[chunk, g, :, CHUNK:]
                carried[...] = across(by) * carried[...] + earlier[chunk, g, :, :CHUNK]

        @pl.when(group > 0)
        def _():
            before = carried[...]
            for m in range(chips):
                back[chunk, m] += across(spread[chunk, m]) * before
            give_all(chunk)

    def write(chunk, which, values):
        at = pl.ds(pl.multiple_of((2 * chunk + which) * ROWS, ROWS), ROWS)
        for j in range(COLS // CHUNK):
            out_ref[at, j * CHUNK : (j + 1) * CHUNK] = values[j * ROWS : (j + 1) * ROWS]

    def pass_on(chunk):
        for k in range(1, chips):
            give(chunk, k, False).wait_recv()
        before = prefix[chunk].reshape(half, CHUNK)
        a, b = own[chunk, mine_at, :CHUNK], other[chunk, :, :CHUNK]
        fa, fb = own[chunk, mine_at, CHUNK:], other[chunk, :, CHUNK:]
        after = across(jnp.where(first, fa, fb)) * before + jnp.where(first, a, b)
        handed[chunk] = jnp.where(first, after, before)
        hand(chunk).start()
        write(chunk, side, jnp.where(first, before, after))

    def take(chunk):
        hand(chunk).wait_recv()
        write(chunk, 1 - side, received[chunk])

    for p in range(2):
        for w in range(windows):
            bins.multiply(w, p)
    bins.settle_first()
    pl.semaphore_wait(barrier, len(peers))
    swap_sides(0).start()
    for w in range(windows):
        if w == windows - 1:
            combine(0)
        bins.multiply(w, 2)
    bins.settle_second()
    swap_sides(1).start()
    bins.close()
    combine(1)
    for chunk in range(chunks):
        scan_group(chunk)
    for chunk in range(chunks):
        finish_groups(chunk)
    for chunk in range(chunks):
        pass_on(chunk)
    for chunk in range(chunks):
        take(chunk)

    for chunk in range(chunks):
        swap_sides(chunk).wait_send()
        hand(chunk).wait_send()
        for k in range(1, chips):
            go(chunk, k, True).wait_send()
            give(chunk, k, True).wait_send()
        for k in range(1, groups):

            @pl.when(group + k < groups)
            def _():
                up(chunk, k, group).wait_send()


def before_own(n, place, where_, weigh, spare, fact):
    windows = spare.shape[0]
    size = max(s for s in range(2, 2 * SLOTS // (2 * SUB) + 1, 2) if n % s == 0 and SLOTS % (s * SUB) == 0)
    groups, chips = n // size, size // 2
    half, chunks = COLS // CHUNK * ROWS, IMAGE_LAYERS // 2
    piece = half // chips
    wide = CHUNK + LANES
    dma = pltpu.SemaphoreType.DMA
    f32 = lambda *shape: pltpu.VMEM(shape, jnp.float32)
    return pl.pallas_call(
        functools.partial(scan_kernel, n, size),
        out_shape=(
            jax.ShapeDtypeStruct((windows, SLOTS, COLS), jnp.float32),
            jax.ShapeDtypeStruct((SLOTS, COLS), jnp.float32),
        ),
        in_specs=[pl.BlockSpec(memory_space=pltpu.VMEM)] * 5,
        out_specs=[pl.BlockSpec(memory_space=pltpu.VMEM)] * 2,
        scratch_shapes=[
            pltpu.VMEM((2, 256, 256), jnp.bfloat16),
            f32(chunks, 2 * half, wide), f32(chunks, half, wide), f32(chunks, chips, piece, wide),
            f32(chunks, chips, piece, wide), f32(chunks, piece, wide), f32(chunks, groups, piece, wide),
            f32(piece, CHUNK), f32(chunks, chips, piece, LANES), f32(chunks, chips, piece, CHUNK),
            f32(chunks, chips, piece, CHUNK), f32(chunks, half, CHUNK), f32(chunks, half, CHUNK),
            dma((chunks,)), dma((chunks,)), dma((chunks, chips)), dma((chunks, chips)),
            dma((chunks, groups)), dma((chunks, groups)), dma((chunks, chips)), dma((chunks, chips)),
            dma((chunks,)), dma((chunks,)),
        ],
        compiler_params=pltpu.CompilerParams(collective_id=0, has_side_effects=True, vmem_limit_bytes=16 * 2**20),
    )(place, where_, weigh, spare, fact)


def heat_kernel(running_ref, before_ref, fact_ref, out_hbm, out_ref, sem):
    windows = running_ref.shape[0]
    stores = []
    for channel in range(IMAGE_LAYERS):
        at = slice(channel * ROWS, (channel + 1) * ROWS)
        for window in range(windows):
            factor = jnp.concatenate([fact_ref[window, channel : channel + 1, :]] * (COLS // LANES), axis=1)
            out_ref[window, at] = factor * before_ref[at] + running_ref[window, at]
            stores.append(
                pltpu.make_async_copy(out_ref.at[window, at], out_hbm.at[window, at], sem.at[window, channel])
            )
            stores[-1].start()
    for store in stores:
        store.wait()


def heat(running, before, fact):
    windows = running.shape[0]
    return pl.pallas_call(
        heat_kernel,
        out_shape=jax.ShapeDtypeStruct(running.shape, jnp.float32),
        in_specs=[pl.BlockSpec(memory_space=pltpu.VMEM)] * 3,
        out_specs=pl.BlockSpec(memory_space=pltpu.HBM),
        scratch_shapes=[pltpu.VMEM(running.shape, jnp.float32), pltpu.SemaphoreType.DMA((windows, IMAGE_LAYERS))],
        compiler_params=pltpu.CompilerParams(vmem_limit_bytes=8 * 2**20),
    )(running, before, fact)


def local(n, point_rows, point_cols, point_chans, point_weights, decay):
    *points, fact = binned(point_rows, point_cols, point_chans, point_weights, decay)
    running, before = before_own(n, *points, fact)
    return heat(running, before, fact).reshape(-1, IMAGE_LAYERS, ROWS, COLS)


def solution(mesh):
    placed = (P("win", None),) * 5
    return jax.shard_map(
        functools.partial(local, mesh.shape["win"]),
        mesh=mesh, in_specs=placed, out_specs=P("win", None, None, None), check_vma=False,
    )
```

```python
import functools
import jax, jax.numpy as jnp
from jax import lax
from jax.experimental import pallas as pl
from jax.experimental.pallas import tpu as pltpu
from jax.sharding import PartitionSpec as P
IMAGE_LAYERS=4
SLOTS=128; ROWS=32; COLS=1024; PART=256; LANES=128; SUB=8
PARTS=2
UNROLL=16
STEP=2*UNROLL
def hot(index, on):
    spread = jnp.broadcast_to(index, (16, LANES)).astype(jnp.bfloat16)
    slots = lax.broadcasted_iota(jnp.int32, (16, LANES), 0).astype(jnp.float32).astype(jnp.bfloat16)
    off = jnp.zeros((16, LANES), jnp.bfloat16)
    return jnp.concatenate([jnp.where(spread == slots + jnp.bfloat16(16.0*g), on, off) for g in range(16)], axis=0)

def swap(x, bits):
    sub = lax.broadcasted_iota(jnp.int32, (SUB, LANES), 0)
    return jnp.take_along_axis(x, sub ^ bits, axis=0)

def exchange(xs, i, j):
    xs[i], xs[j] = jnp.minimum(xs[i], xs[j]), jnp.maximum(xs[i], xs[j])

def sort_rows(xs):
    n=len(xs); xs=list(xs)
    sub = lax.broadcasted_iota(jnp.int32, (SUB, LANES), 0)
    k=2
    while k<=n:
        for b in range(0,n,k):
            for t in range(k//2): exchange(xs,b+t,b+k-1-t)
        d=k//4
        while d:
            for i in range(n):
                if not i & d: exchange(xs,i,i+d)
            d//=2
        k*=2
    width=1
    while width<SUB:
        low = (sub & width)==0
        ys=[swap(x,2*width-1) for x in xs]
        xs=[jnp.where(low,jnp.minimum(xs[i],ys[n-1-i]),jnp.maximum(xs[i],ys[n-1-i])) for i in range(n)]
        d=width//2
        while d:
            low=(sub & d)==0
            xs=[jnp.where(low,jnp.minimum(x,y),jnp.maximum(x,y)) for x,y in ((x,swap(x,d)) for x in xs)]
            d//=2
        d=n//2
        while d:
            for i in range(n):
                if not i & d: exchange(xs,i,i+d)
            d//=2
        width*=2
    return xs

def splits(height):
    first, second = (height * cut // 8 // STEP * STEP for cut in (3, 5))
    return (0, first, second, height)


def right(where_, weigh, r):
    return jnp.concatenate([hot(where_[pl.ds(r+i,1),:],jnp.broadcast_to(weigh[pl.ds(r+i,1),:],(16,LANES)).astype(jnp.bfloat16)) for i in range(2)],axis=1)


def left(place, r, base):
    one=jnp.ones((16,LANES),jnp.bfloat16)
    return jnp.concatenate([hot(place[pl.ds(r+i,1),:]-base,one) for i in range(2)],axis=1)


def blocks(got, quarter):
    for block in range(8):
        index=4*quarter+block
        part,j,c=index//8,index//2%4,index%2
        yield slice(64*part+32*c,64*part+32*c+32),slice(256*j,256*j+256),2*part+c,got[32*block:32*block+32]


def kernel(rows_hbm, cols_hbm, chans_hbm, weights_hbm, decay_hbm, place, where_, weigh, spare, fact, rows, cols, chans, weights, decay, keys, odd, sem):
    copies=[pltpu.make_async_copy(a,b,sem.at[i]) for i,(a,b) in enumerate(((decay_hbm,decay),(weights_hbm,weights),(cols_hbm,cols),(chans_hbm,chans),(rows_hbm,rows)))]
    for copy in copies: copy.start()
    windows = spare.shape[0]
    spare[...] = jnp.zeros(spare.shape, jnp.float32)
    for copy in copies: copy.wait()
    pl.run_scoped(functools.partial(sort_points,rows,cols,chans,weights,decay,place,where_,weigh,spare,fact,keys,odd),
        *[pltpu.ACC(m)((256,256),jnp.float32) for m in range(2)])


def sort_points(rows, cols, chans, weights, decay, place, where_, weigh, spare, fact, keys, odd, *accs):
    windows = spare.shape[0]
    for channel in range(IMAGE_LAYERS):
        factor = jnp.float32(1.0)
        for w in range(windows):
            factor = factor * decay[w, channel]
            fact[w, channel : channel + 1, :] = jnp.full((1, LANES), factor, jnp.float32)
            at = IMAGE_LAYERS + channel
            fact[w, at : at + 1, :] = jnp.full((1, LANES), decay[w, channel], jnp.float32)
    total = rows.shape[0]; height = total//windows
    _, first, second, _ = splits(height)
    for v in range(total//16):
        at=pl.ds(16*v,16)
        c=cols[at,:]; k=chans[at,:]
        w=(weights[at,:].astype(jnp.float32)*512.0).astype(jnp.int32)
        lidx=((k>>1)<<8)|((c>>8)<<6)|((k&1)<<5)|rows[at,:]
        keys[at,:]=(lidx<<20)|((c&255)<<12)|w
    n=height//SUB
    ranks=lax.broadcasted_iota(jnp.int32,(SUB,LANES),0)*n
    bounds=[]
    for w in range(windows):
        xs=[keys[pl.ds(w+windows*SUB*v,SUB,stride=windows),:] for v in range(n)]
        xs=sort_rows(xs)
        least=jnp.full((SUB,LANES),height,jnp.int32); most=jnp.full((SUB,LANES),-1,jnp.int32)
        for v in range(n):
            x=xs[v]
            index=x>>20
            rank=ranks+v
            base=jnp.where(rank<first,0,jnp.where(rank<second,128,256))
            out_of=(index<base)|(index>=base+256)
            least=jnp.minimum(least,jnp.where(out_of,rank,height))
            most=jnp.maximum(most,jnp.where(out_of,rank,-1))
            at=pl.ds(w*height+v,SUB,stride=n)
            index=index.astype(jnp.float32)
            place[at,:]=index
            odd[at,:]=jnp.where(out_of,index,-1000.0)
            where_[at,:]=((x>>12)&255).astype(jnp.float32)
            weigh[at,:]=(x&4095).astype(jnp.float32)*(1.0/512.0)
        bounds.append((jnp.min(least),jnp.max(most)))
    rest=slice(total,place.shape[0]); size=(place.shape[0]-total,LANES)
    place[rest,:]=jnp.full(size,-1000.0,jnp.float32)
    where_[rest,:]=jnp.zeros(size,jnp.float32)
    weigh[rest,:]=jnp.zeros(size,jnp.float32)
    for w in range(windows):
        least,most=bounds[w]

        @pl.when(most>=least)
        def _():
            begin=(least>>2)<<2
            for quarter in (0,2):
                for m in range(2): pltpu.matmul_pop(accs[m])

                def body(i,c):
                    for m in range(2):
                        r=w*height+begin+4*i+2*m
                        pltpu.matmul_push_rhs(right(where_,weigh,r),staging_register=0,mxu_index=m,transpose=True)
                        pltpu.matmul_acc_lhs(accs[m],left(odd,r,128.0*quarter),load_staged_rhs=0)
                    return c
                lax.fori_loop(0,(most-begin)//4+1,body,0)
                for at,across_,_,piece in blocks(pltpu.matmul_pop(accs[0])+pltpu.matmul_pop(accs[1]),quarter):
                    spare[w,at,across_]=piece


def view(x):
    windows,count=x.shape
    return x.reshape(windows,count//LANES,LANES).transpose(1,0,2).reshape(windows*count//LANES,LANES)
def binned(r,c,k,w,d):
    windows,count=r.shape
    height=count//LANES
    tall=windows*height
    points=jax.ShapeDtypeStruct((tall+SUB,LANES),jnp.float32)
    return pl.pallas_call(
        kernel,
        out_shape=(
            points, points, points,
            jax.ShapeDtypeStruct((windows, SLOTS, COLS), jnp.float32),
            jax.ShapeDtypeStruct((windows, SUB, LANES), jnp.float32),
        ),
        in_specs=[pl.BlockSpec(memory_space=pltpu.HBM)] * 5,
        out_specs=[pl.BlockSpec(memory_space=pltpu.VMEM)] * 5,
        scratch_shapes=[pltpu.VMEM((tall, LANES), jnp.int32)] * 3
        + [pltpu.VMEM((tall, LANES), jnp.bfloat16), pltpu.SMEM(d.shape, jnp.float32)]
        + [pltpu.VMEM((tall, LANES), jnp.int32), pltpu.VMEM((tall, LANES), jnp.float32)]
        + [pltpu.SemaphoreType.DMA((5,))],
        compiler_params=pltpu.CompilerParams(vmem_limit_bytes=16 * 2**20),
    )(*(pltpu.with_memory_space_constraint(x, pltpu.HBM) for x in (*map(view, (r, c, k, w)), d)))


MESH = pl.DeviceIdType.MESH
CHUNK = 512


def across(tile):
    return jnp.concatenate([tile] * (CHUNK // LANES), axis=1)


class Bins:
    def __init__(self, place, where_, weigh, spare, fact, running, ahead, own, unused, accs):
        self.refs = place, where_, weigh
        self.spare, self.fact, self.running, self.ahead, self.own, self.unused = spare, fact, running, ahead, own, unused
        self.accs = accs
        self.windows = running.shape[0]
        self.height = (place.shape[0] - SUB) // self.windows
        self.cuts = splits(self.height)
        self.order = [(w, p) for p in range(3) for w in range(self.windows)]
        for acc in accs:
            unused[:, :PART] = pltpu.matmul_pop(acc)[: unused.shape[0]]
        for m in range(2):
            self.push(m, 0, self.start(0) + 2 * m)
            ahead[m] = left(place, self.start(0) + 2 * m, jnp.float32(0.0))

    def start(self, k):
        w, p = self.order[k % len(self.order)]
        return w * self.height + self.cuts[p]

    def push(self, m, staging, r):
        pltpu.matmul_push_rhs(right(*self.refs[1:], r), staging_register=staging, mxu_index=m, transpose=True)

    def region(self, w, p):
        at = 2 * (w + self.windows * (p % 2))
        return self.accs[at : at + 2]

    def multiply(self, w, p):
        k = self.order.index((w, p))
        trips = (self.cuts[p + 1] - self.cuts[p]) // STEP
        base, then = 128.0 * p, 128.0 * self.order[(k + 1) % len(self.order)][1]

        def body(i, carry):
            for u in range(UNROLL):
                m, s = u % 2, u // 2 % 2
                r = self.start(k) + i * STEP + 2 * u
                ending = u >= UNROLL - 2
                later = jnp.where(i == trips - 1, self.start(k + 1) + 2 * m, r + 4) if ending else r + 4
                self.push(m, 1 - s, later)
                hot_left = self.ahead[m] if u < 2 else left(self.refs[0], r, base)
                pltpu.matmul_acc_lhs(self.region(w, p)[m], hot_left, load_staged_rhs=s)
                if ending:
                    self.ahead[m] = left(self.refs[0], later, jnp.where(i == trips - 1, then, base))
            return carry

        lax.fori_loop(0, trips, body, 0)

    def pop(self, w, p):
        first, second = self.region(w, p)
        got = pltpu.matmul_pop(first) + pltpu.matmul_pop(second)
        return [got[32 * b : 32 * b + 32] for b in range(8)]

    def settle(self, part, w, pieces):
        for b, piece in enumerate(pieces):
            j, c = b // 2, b % 2
            channel = 2 * part + c
            at, wide = slice(ROWS * channel, ROWS * channel + ROWS), slice(PART * j, PART * j + PART)
            piece = piece + self.spare[w, at, wide]
            if w:
                row = self.fact[w, IMAGE_LAYERS + channel : IMAGE_LAYERS + channel + 1, :]
                piece = jnp.concatenate([row] * (PART // LANES), axis=1) * self.running[w - 1, at, wide] + piece
            self.running[w, at, wide] = piece
            if w == self.windows - 1:
                per = CHUNK // PART
                down = c * (COLS // CHUNK) * ROWS + j // per * ROWS
                self.own[part, down : down + ROWS, j % per * PART : (j % per + 1) * PART] = piece

    def settle_first(self):
        for w in range(self.windows):
            outer, inner = self.pop(w, 0), self.pop(w, 1)
            self.settle(0, w, outer[:4] + [x + y for x, y in zip(outer[4:], inner[:4])])
            for b, piece in enumerate(inner[4:]):
                at = (2 + b % 2) * ROWS
                self.running[w, at : at + ROWS, b // 2 * PART : (b // 2 + 1) * PART] = piece

    def settle_second(self):
        for w in range(self.windows):
            pieces = self.pop(w, 2)
            for b in range(4):
                at = (2 + b % 2) * ROWS
                pieces[b] = pieces[b] + self.running[w, at : at + ROWS, b // 2 * PART : (b // 2 + 1) * PART]
            self.settle(1, w, pieces)

    def close(self):
        for m in range(2):
            pltpu.matmul_acc_lhs(self.accs[m], jnp.zeros((256, 256), jnp.bfloat16), load_staged_rhs=0)
            self.unused[:, :PART] = pltpu.matmul_pop(self.accs[m])[: self.unused.shape[0]]


def scan_kernel(n, size, *refs):
    windows = refs[5].shape[0]
    pl.run_scoped(
        lambda *accs: scan(n, size, accs, *refs),
        *[pltpu.ACC(m)((256, PART), jnp.float32) for _ in range(2 * windows) for m in range(2)],
    )


def scan(
    n, size, accs, place, where_, weigh, spare, fact_ref, running_ref, out_ref,
    ahead, own, other, stage, inbox, total, earlier, carried, spread, back, prefix, handed, received,
    swap_send, swap_recv, go_send, go_recv, up_send, up_recv, back_send, back_recv, hand_send, hand_recv,
):
    windows = running_ref.shape[0]
    groups, chips = n // size, size // 2
    half = COLS // CHUNK * ROWS
    piece = half // chips
    chunks = IMAGE_LAYERS // 2
    me = lax.axis_index("win")
    group, member = lax.div(me, size), lax.rem(me, size)
    chip, side = lax.div(member, 2), lax.rem(member, 2)
    partner = me + 1 - 2 * side
    mate = lambda k: group * size + 2 * lax.rem(chip + k, chips) + side
    counter = lambda k: lax.rem(me + k * size, n)

    barrier = pltpu.get_barrier_semaphore()
    peers = [partner] + [mate(k) for k in range(1, chips)] + [counter(k) for k in range(1, groups)]
    for peer in peers:
        pl.semaphore_signal(barrier, inc=1, device_id=(peer,), device_id_type=MESH)
    for channel in range(IMAGE_LAYERS):
        factor = fact_ref[windows - 1, channel : channel + 1, :]
        down = channel % 2 * half
        own[channel // 2, down : down + half, CHUNK:] = jnp.broadcast_to(factor, (half, LANES))
    bins = Bins(place, where_, weigh, spare, fact_ref, running_ref, ahead, own, carried, accs)

    def remote(src, dst, send, recv, device):
        return pltpu.make_async_remote_copy(
            src_ref=src, dst_ref=dst, send_sem=send, recv_sem=recv, device_id=(device,), device_id_type=MESH
        )

    def swap_sides(chunk):
        away = own.at[chunk, pl.ds(pl.multiple_of((1 - side) * half, half), half)]
        return remote(
            away, other.at[chunk], swap_send.at[chunk], swap_recv.at[chunk], partner
        )

    def go(chunk, k, sender):
        peer = lax.rem(chip + k, chips)
        slot = chip if sender else peer
        return remote(
            stage.at[chunk, peer], inbox.at[chunk, slot],
            go_send.at[chunk, k], go_recv.at[chunk, slot], mate(k),
        )

    def up(chunk, k, slot):
        return remote(
            total.at[chunk], earlier.at[chunk, slot],
            up_send.at[chunk, k], up_recv.at[chunk, slot], counter(k),
        )

    def give(chunk, k, sender):
        peer = lax.rem(chip + k, chips)
        slot = chip if sender else peer
        return remote(
            back.at[chunk, peer], prefix.at[chunk, slot], back_send.at[chunk, k], back_recv.at[chunk, slot], mate(k)
        )

    def hand(chunk):
        return remote(
            handed.at[chunk], received.at[chunk], hand_send.at[chunk], hand_recv.at[chunk], partner
        )

    first = side == 0
    mine_at = pl.ds(pl.multiple_of(side * half, half), half)

    def combine(chunk):
        swap_sides(chunk).wait_recv()
        a, b = own[chunk, mine_at, :CHUNK], other[chunk, :, :CHUNK]
        fa, fb = own[chunk, mine_at, CHUNK:], other[chunk, :, CHUNK:]
        late = across(jnp.where(first, fb, fa))
        both = late * jnp.where(first, a, b) + jnp.where(first, b, a)
        for p in range(chips):
            stage[chunk, p, :, :CHUNK] = both[p * piece : (p + 1) * piece]
            stage[chunk, p, :, CHUNK:] = (fa * fb)[p * piece : (p + 1) * piece]
        for k in range(1, chips):
            go(chunk, k, True).start()
        inbox[chunk, chip] = stage[chunk, chip]

    def give_all(chunk):
        for k in range(1, chips):
            give(chunk, k, True).start()
        prefix[chunk, chip] = back[chunk, chip]

    def scan_group(chunk):
        for k in range(1, chips):
            go(chunk, k, False).wait_recv()
        running = jnp.zeros((piece, CHUNK), jnp.float32)
        factor = jnp.ones((piece, LANES), jnp.float32)
        for m in range(chips):
            back[chunk, m] = running
            by = inbox[chunk, m, :, CHUNK:]
            spread[chunk, m] = factor
            running = across(by) * running + inbox[chunk, m, :, :CHUNK]
            factor = factor * by
        total[chunk, :, :CHUNK] = running
        total[chunk, :, CHUNK:] = factor
        for k in range(1, groups):

            @pl.when(group + k < groups)
            def _():
                up(chunk, k, group).start()

        @pl.when(group == 0)
        def _():
            give_all(chunk)

    def finish_groups(chunk):
        if groups == 1:
            return
        carried[...] = jnp.zeros((piece, CHUNK), jnp.float32)
        for g in range(groups - 1):

            @pl.when(g < group)
            def _():
                up(chunk, 1, g).wait_recv()
                by = earlier[chunk, g, :, CHUNK:]
                carried[...] = across(by) * carried[...] + earlier[chunk, g, :, :CHUNK]

        @pl.when(group > 0)
        def _():
            before = carried[...]
            for m in range(chips):
                back[chunk, m] += across(spread[chunk, m]) * before
            give_all(chunk)

    def write(chunk, which, values):
        at = pl.ds(pl.multiple_of((2 * chunk + which) * ROWS, ROWS), ROWS)
        for j in range(COLS // CHUNK):
            out_ref[at, j * CHUNK : (j + 1) * CHUNK] = values[j * ROWS : (j + 1) * ROWS]

    def pass_on(chunk):
        for k in range(1, chips):
            give(chunk, k, False).wait_recv()
        before = prefix[chunk].reshape(half, CHUNK)
        a, b = own[chunk, mine_at, :CHUNK], other[chunk, :, :CHUNK]
        fa, fb = own[chunk, mine_at, CHUNK:], other[chunk, :, CHUNK:]
        after = across(jnp.where(first, fa, fb)) * before + jnp.where(first, a, b)
        handed[chunk] = jnp.where(first, after, before)
        hand(chunk).start()
        write(chunk, side, jnp.where(first, before, after))

    def take(chunk):
        hand(chunk).wait_recv()
        write(chunk, 1 - side, received[chunk])

    for p in range(2):
        for w in range(windows):
            bins.multiply(w, p)
    bins.settle_first()
    pl.semaphore_wait(barrier, len(peers))
    swap_sides(0).start()
    for w in range(windows):
        if w == windows - 1:
            combine(0)
        bins.multiply(w, 2)
    bins.settle_second()
    swap_sides(1).start()
    bins.close()
    combine(1)
    for chunk in range(chunks):
        scan_group(chunk)
    for chunk in range(chunks):
        finish_groups(chunk)
    for chunk in range(chunks):
        pass_on(chunk)
    for chunk in range(chunks):
        take(chunk)

    for chunk in range(chunks):
        swap_sides(chunk).wait_send()
        hand(chunk).wait_send()
        for k in range(1, chips):
            go(chunk, k, True).wait_send()
            give(chunk, k, True).wait_send()
        for k in range(1, groups):

            @pl.when(group + k < groups)
            def _():
                up(chunk, k, group).wait_send()


def before_own(n, place, where_, weigh, spare, fact):
    windows = spare.shape[0]
    size = max(s for s in range(2, 2 * SLOTS // (2 * SUB) + 1, 2) if n % s == 0 and SLOTS % (s * SUB) == 0)
    groups, chips = n // size, size // 2
    half, chunks = COLS // CHUNK * ROWS, IMAGE_LAYERS // 2
    piece = half // chips
    wide = CHUNK + LANES
    dma = pltpu.SemaphoreType.DMA
    f32 = lambda *shape: pltpu.VMEM(shape, jnp.float32)
    return pl.pallas_call(
        functools.partial(scan_kernel, n, size),
        out_shape=(
            jax.ShapeDtypeStruct((windows, SLOTS, COLS), jnp.float32),
            jax.ShapeDtypeStruct((SLOTS, COLS), jnp.float32),
        ),
        in_specs=[pl.BlockSpec(memory_space=pltpu.VMEM)] * 5,
        out_specs=[pl.BlockSpec(memory_space=pltpu.VMEM)] * 2,
        scratch_shapes=[
            pltpu.VMEM((2, 256, 256), jnp.bfloat16),
            f32(chunks, 2 * half, wide), f32(chunks, half, wide), f32(chunks, chips, piece, wide),
            f32(chunks, chips, piece, wide), f32(chunks, piece, wide), f32(chunks, groups, piece, wide),
            f32(piece, CHUNK), f32(chunks, chips, piece, LANES), f32(chunks, chips, piece, CHUNK),
            f32(chunks, chips, piece, CHUNK), f32(chunks, half, CHUNK), f32(chunks, half, CHUNK),
            dma((chunks,)), dma((chunks,)), dma((chunks, chips)), dma((chunks, chips)),
            dma((chunks, groups)), dma((chunks, groups)), dma((chunks, chips)), dma((chunks, chips)),
            dma((chunks,)), dma((chunks,)),
        ],
        compiler_params=pltpu.CompilerParams(collective_id=0, has_side_effects=True, vmem_limit_bytes=16 * 2**20),
    )(place, where_, weigh, spare, fact)


def heat_kernel(running_ref, before_ref, fact_ref, out_hbm, out_ref, sem):
    windows = running_ref.shape[0]
    stores = []
    for channel in range(IMAGE_LAYERS):
        at = slice(channel * ROWS, (channel + 1) * ROWS)
        for window in range(windows):
            factor = jnp.concatenate([fact_ref[window, channel : channel + 1, :]] * (COLS // LANES), axis=1)
            out_ref[window, at] = factor * before_ref[at] + running_ref[window, at]
            stores.append(
                pltpu.make_async_copy(out_ref.at[window, at], out_hbm.at[window, at], sem.at[window, channel])
            )
            stores[-1].start()
    for store in stores:
        store.wait()


def heat(running, before, fact):
    windows = running.shape[0]
    return pl.pallas_call(
        heat_kernel,
        out_shape=jax.ShapeDtypeStruct(running.shape, jnp.float32),
        in_specs=[pl.BlockSpec(memory_space=pltpu.VMEM)] * 3,
        out_specs=pl.BlockSpec(memory_space=pltpu.HBM),
        scratch_shapes=[pltpu.VMEM(running.shape, jnp.float32), pltpu.SemaphoreType.DMA((windows, IMAGE_LAYERS))],
        compiler_params=pltpu.CompilerParams(vmem_limit_bytes=8 * 2**20),
    )(running, before, fact)


def local(n, point_rows, point_cols, point_chans, point_weights, decay):
    *points, fact = binned(point_rows, point_cols, point_chans, point_weights, decay)
    running, before = before_own(n, *points, fact)
    return heat(running, before, fact).reshape(-1, IMAGE_LAYERS, ROWS, COLS)


def solution(mesh):
    placed = (P("win", None),) * 5
    return jax.shard_map(
        functools.partial(local, mesh.shape["win"]),
        mesh=mesh, in_specs=placed, out_specs=P("win", None, None, None), check_vma=False,
    )
```

```python
import functools
import jax, jax.numpy as jnp
from jax import lax
from jax.experimental import pallas as pl
from jax.experimental.pallas import tpu as pltpu
from jax.sharding import PartitionSpec as P
IMAGE_LAYERS=4
SLOTS=128; ROWS=32; COLS=1024; PART=256; LANES=128; SUB=8
PARTS=2
UNROLL=16
STEP=2*UNROLL
def hot(index, on):
    spread = jnp.broadcast_to(index, (16, LANES)).astype(jnp.bfloat16)
    slots = lax.broadcasted_iota(jnp.int32, (16, LANES), 0).astype(jnp.float32).astype(jnp.bfloat16)
    off = jnp.zeros((16, LANES), jnp.bfloat16)
    return jnp.concatenate([jnp.where(spread == slots + jnp.bfloat16(16.0*g), on, off) for g in range(16)], axis=0)

def swap(x, bits):
    sub = lax.broadcasted_iota(jnp.int32, (SUB, LANES), 0)
    return jnp.take_along_axis(x, sub ^ bits, axis=0)

def exchange(xs, i, j):
    xs[i], xs[j] = jnp.minimum(xs[i], xs[j]), jnp.maximum(xs[i], xs[j])

def sort_rows(xs):
    n=len(xs); xs=list(xs)
    sub = lax.broadcasted_iota(jnp.int32, (SUB, LANES), 0)
    k=2
    while k<=n:
        for b in range(0,n,k):
            for t in range(k//2): exchange(xs,b+t,b+k-1-t)
        d=k//4
        while d:
            for i in range(n):
                if not i & d: exchange(xs,i,i+d)
            d//=2
        k*=2
    width=1
    while width<SUB:
        low = (sub & width)==0
        ys=[swap(x,2*width-1) for x in xs]
        xs=[jnp.where(low,jnp.minimum(xs[i],ys[n-1-i]),jnp.maximum(xs[i],ys[n-1-i])) for i in range(n)]
        d=width//2
        while d:
            low=(sub & d)==0
            xs=[jnp.where(low,jnp.minimum(x,y),jnp.maximum(x,y)) for x,y in ((x,swap(x,d)) for x in xs)]
            d//=2
        d=n//2
        while d:
            for i in range(n):
                if not i & d: exchange(xs,i,i+d)
            d//=2
        width*=2
    return xs

def splits(height):
    first, second = (height * cut // 8 // STEP * STEP for cut in (3, 5))
    return (0, first, second, height)


def right(where_, weigh, r):
    return jnp.concatenate([hot(where_[pl.ds(r+i,1),:],jnp.broadcast_to(weigh[pl.ds(r+i,1),:],(16,LANES)).astype(jnp.bfloat16)) for i in range(2)],axis=1)


def left(place, r, base):
    one=jnp.ones((16,LANES),jnp.bfloat16)
    return jnp.concatenate([hot(place[pl.ds(r+i,1),:]-base,one) for i in range(2)],axis=1)


def blocks(got, quarter):
    for block in range(8):
        index=4*quarter+block
        part,j,c=index//8,index//2%4,index%2
        yield slice(64*part+32*c,64*part+32*c+32),slice(256*j,256*j+256),2*part+c,got[32*block:32*block+32]


def kernel(rows_hbm, cols_hbm, chans_hbm, weights_hbm, decay_hbm, place, where_, weigh, spare, fact, rows, cols, chans, weights, decay, keys, odd, sem):
    copies=[pltpu.make_async_copy(a,b,sem.at[i]) for i,(a,b) in enumerate(((decay_hbm,decay),(weights_hbm,weights),(cols_hbm,cols),(chans_hbm,chans),(rows_hbm,rows)))]
    for copy in copies: copy.start()
    windows = spare.shape[0]
    spare[...] = jnp.zeros(spare.shape, jnp.float32)
    for copy in copies: copy.wait()
    pl.run_scoped(functools.partial(sort_points,rows,cols,chans,weights,decay,place,where_,weigh,spare,fact,keys,odd),
        *[pltpu.ACC(m)((256,256),jnp.float32) for m in range(2)])


def sort_points(rows, cols, chans, weights, decay, place, where_, weigh, spare, fact, keys, odd, *accs):
    windows = spare.shape[0]
    for channel in range(IMAGE_LAYERS):
        factor = jnp.float32(1.0)
        for w in range(windows):
            factor = factor * decay[w, channel]
            fact[w, channel : channel + 1, :] = jnp.full((1, LANES), factor, jnp.float32)
            at = IMAGE_LAYERS + channel
            fact[w, at : at + 1, :] = jnp.full((1, LANES), decay[w, channel], jnp.float32)
    total = rows.shape[0]; height = total//windows
    _, first, second, _ = splits(height)
    for v in range(total//16):
        at=pl.ds(16*v,16)
        c=cols[at,:]; k=chans[at,:]
        w=(weights[at,:].astype(jnp.float32)*512.0).astype(jnp.int32)
        lidx=((k>>1)<<8)|((c>>8)<<6)|((k&1)<<5)|rows[at,:]
        keys[at,:]=(lidx<<20)|((c&255)<<12)|w
    n=height//SUB
    ranks=lax.broadcasted_iota(jnp.int32,(SUB,LANES),0)*n
    bounds=[]
    for w in range(windows):
        xs=[keys[pl.ds(w+windows*SUB*v,SUB,stride=windows),:] for v in range(n)]
        xs=sort_rows(xs)
        least=jnp.full((SUB,LANES),height,jnp.int32); most=jnp.full((SUB,LANES),-1,jnp.int32)
        for v in range(n):
            x=xs[v]
            index=x>>20
            rank=ranks+v
            base=jnp.where(rank<first,0,jnp.where(rank<second,128,256))
            out_of=(index<base)|(index>=base+256)
            least=jnp.minimum(least,jnp.where(out_of,rank,height))
            most=jnp.maximum(most,jnp.where(out_of,rank,-1))
            at=pl.ds(w*height+v,SUB,stride=n)
            index=index.astype(jnp.float32)
            place[at,:]=index
            odd[at,:]=jnp.where(out_of,index,-1000.0)
            where_[at,:]=((x>>12)&255).astype(jnp.float32)
            weigh[at,:]=(x&4095).astype(jnp.float32)*(1.0/512.0)
        bounds.append((jnp.min(least),jnp.max(most)))
    rest=slice(total,place.shape[0]); size=(place.shape[0]-total,LANES)
    place[rest,:]=jnp.full(size,-1000.0,jnp.float32)
    where_[rest,:]=jnp.zeros(size,jnp.float32)
    weigh[rest,:]=jnp.zeros(size,jnp.float32)
    for w in range(windows):
        least,most=bounds[w]

        @pl.when(most>=least)
        def _():
            begin=(least>>2)<<2
            for quarter in (0,2):
                for m in range(2): pltpu.matmul_pop(accs[m])

                def body(i,c):
                    for m in range(2):
                        r=w*height+begin+4*i+2*m
                        pltpu.matmul_push_rhs(right(where_,weigh,r),staging_register=0,mxu_index=m,transpose=True)
                        pltpu.matmul_acc_lhs(accs[m],left(odd,r,128.0*quarter),load_staged_rhs=0)
                    return c
                lax.fori_loop(0,(most-begin)//4+1,body,0)
                for at,across_,_,piece in blocks(pltpu.matmul_pop(accs[0])+pltpu.matmul_pop(accs[1]),quarter):
                    spare[w,at,across_]=piece


def view(x):
    windows,count=x.shape
    return x.reshape(windows,count//LANES,LANES).transpose(1,0,2).reshape(windows*count//LANES,LANES)
def binned(r,c,k,w,d):
    windows,count=r.shape
    height=count//LANES
    tall=windows*height
    points=jax.ShapeDtypeStruct((tall+SUB,LANES),jnp.float32)
    return pl.pallas_call(
        kernel,
        out_shape=(
            points, points, points,
            jax.ShapeDtypeStruct((windows, SLOTS, COLS), jnp.float32),
            jax.ShapeDtypeStruct((windows, SUB, LANES), jnp.float32),
        ),
        in_specs=[pl.BlockSpec(memory_space=pltpu.HBM)] * 5,
        out_specs=[pl.BlockSpec(memory_space=pltpu.VMEM)] * 5,
        scratch_shapes=[pltpu.VMEM((tall, LANES), jnp.int32)] * 3
        + [pltpu.VMEM((tall, LANES), jnp.bfloat16), pltpu.SMEM(d.shape, jnp.float32)]
        + [pltpu.VMEM((tall, LANES), jnp.int32), pltpu.VMEM((tall, LANES), jnp.float32)]
        + [pltpu.SemaphoreType.DMA((5,))],
        compiler_params=pltpu.CompilerParams(vmem_limit_bytes=16 * 2**20),
    )(*(pltpu.with_memory_space_constraint(x, pltpu.HBM) for x in (*map(view, (r, c, k, w)), d)))


MESH = pl.DeviceIdType.MESH
CHUNK = 512


def across(tile):
    return jnp.concatenate([tile] * (CHUNK // LANES), axis=1)


class Bins:
    def __init__(self, place, where_, weigh, spare, fact, running, ahead, own, unused, accs):
        self.refs = place, where_, weigh
        self.spare, self.fact, self.running, self.ahead, self.own, self.unused = spare, fact, running, ahead, own, unused
        self.accs = accs
        self.windows = running.shape[0]
        self.height = (place.shape[0] - SUB) // self.windows
        self.cuts = splits(self.height)
        self.order = [(w, p) for p in range(3) for w in range(self.windows)]
        for acc in accs:
            unused[:, :PART] = pltpu.matmul_pop(acc)[: unused.shape[0]]
        for m in range(2):
            self.push(m, 0, self.start(0) + 2 * m)
            ahead[m] = left(place, self.start(0) + 2 * m, jnp.float32(0.0))

    def start(self, k):
        w, p = self.order[k % len(self.order)]
        return w * self.height + self.cuts[p]

    def push(self, m, staging, r):
        pltpu.matmul_push_rhs(right(*self.refs[1:], r), staging_register=staging, mxu_index=m, transpose=True)

    def region(self, w, p):
        at = 2 * (w + self.windows * (p % 2))
        return self.accs[at : at + 2]

    def multiply(self, w, p):
        k = self.order.index((w, p))
        trips = (self.cuts[p + 1] - self.cuts[p]) // STEP
        base, then = 128.0 * p, 128.0 * self.order[(k + 1) % len(self.order)][1]

        def body(i, carry):
            for u in range(UNROLL):
                m, s = u % 2, u // 2 % 2
                r = self.start(k) + i * STEP + 2 * u
                ending = u >= UNROLL - 2
                later = jnp.where(i == trips - 1, self.start(k + 1) + 2 * m, r + 4) if ending else r + 4
                self.push(m, 1 - s, later)
                hot_left = self.ahead[m] if u < 2 else left(self.refs[0], r, base)
                pltpu.matmul_acc_lhs(self.region(w, p)[m], hot_left, load_staged_rhs=s)
                if ending:
                    self.ahead[m] = left(self.refs[0], later, jnp.where(i == trips - 1, then, base))
            return carry

        lax.fori_loop(0, trips, body, 0)

    def pop(self, w, p):
        first, second = self.region(w, p)
        got = pltpu.matmul_pop(first) + pltpu.matmul_pop(second)
        return [got[32 * b : 32 * b + 32] for b in range(8)]

    def settle(self, part, w, pieces):
        for b, piece in enumerate(pieces):
            j, c = b // 2, b % 2
            channel = 2 * part + c
            at, wide = slice(ROWS * channel, ROWS * channel + ROWS), slice(PART * j, PART * j + PART)
            piece = piece + self.spare[w, at, wide]
            if w:
                row = self.fact[w, IMAGE_LAYERS + channel : IMAGE_LAYERS + channel + 1, :]
                piece = jnp.concatenate([row] * (PART // LANES), axis=1) * self.running[w - 1, at, wide] + piece
            self.running[w, at, wide] = piece
            if w == self.windows - 1:
                per = CHUNK // PART
                down = c * (COLS // CHUNK) * ROWS + j // per * ROWS
                self.own[part, down : down + ROWS, j % per * PART : (j % per + 1) * PART] = piece

    def settle_first(self):
        for w in range(self.windows):
            outer, inner = self.pop(w, 0), self.pop(w, 1)
            self.settle(0, w, outer[:4] + [x + y for x, y in zip(outer[4:], inner[:4])])
            for b, piece in enumerate(inner[4:]):
                at = (2 + b % 2) * ROWS
                self.running[w, at : at + ROWS, b // 2 * PART : (b // 2 + 1) * PART] = piece

    def settle_second(self):
        for w in range(self.windows):
            pieces = self.pop(w, 2)
            for b in range(4):
                at = (2 + b % 2) * ROWS
                pieces[b] = pieces[b] + self.running[w, at : at + ROWS, b // 2 * PART : (b // 2 + 1) * PART]
            self.settle(1, w, pieces)

    def close(self):
        for m in range(2):
            pltpu.matmul_acc_lhs(self.accs[m], jnp.zeros((256, 256), jnp.bfloat16), load_staged_rhs=0)
            self.unused[:, :PART] = pltpu.matmul_pop(self.accs[m])[: self.unused.shape[0]]


def scan_kernel(n, size, *refs):
    windows = refs[5].shape[0]
    pl.run_scoped(
        lambda *accs: scan(n, size, accs, *refs),
        *[pltpu.ACC(m)((256, PART), jnp.float32) for _ in range(2 * windows) for m in range(2)],
    )


def scan(
    n, size, accs, place, where_, weigh, spare, fact_ref, running_ref, out_ref,
    ahead, own, other, stage, inbox, total, earlier, carried, spread, back, prefix, handed, received,
    swap_send, swap_recv, go_send, go_recv, up_send, up_recv, back_send, back_recv, hand_send, hand_recv,
):
    windows = running_ref.shape[0]
    groups, chips = n // size, size // 2
    half = COLS // CHUNK * ROWS
    piece = half // chips
    chunks = IMAGE_LAYERS // 2
    me = lax.axis_index("win")
    group, member = lax.div(me, size), lax.rem(me, size)
    chip, side = lax.div(member, 2), lax.rem(member, 2)
    partner = me + 1 - 2 * side
    mate = lambda k: group * size + 2 * lax.rem(chip + k, chips) + side
    counter = lambda k: lax.rem(me + k * size, n)

    barrier = pltpu.get_barrier_semaphore()
    peers = [partner] + [mate(k) for k in range(1, chips)] + [counter(k) for k in range(1, groups)]
    for peer in peers:
        pl.semaphore_signal(barrier, inc=1, device_id=(peer,), device_id_type=MESH)
    for channel in range(IMAGE_LAYERS):
        factor = fact_ref[windows - 1, channel : channel + 1, :]
        down = channel % 2 * half
        own[channel // 2, down : down + half, CHUNK:] = jnp.broadcast_to(factor, (half, LANES))
    bins = Bins(place, where_, weigh, spare, fact_ref, running_ref, ahead, own, carried, accs)

    def remote(src, dst, send, recv, device):
        return pltpu.make_async_remote_copy(
            src_ref=src, dst_ref=dst, send_sem=send, recv_sem=recv, device_id=(device,), device_id_type=MESH
        )

    def swap_sides(chunk):
        away = own.at[chunk, pl.ds(pl.multiple_of((1 - side) * half, half), half)]
        return remote(
            away, other.at[chunk], swap_send.at[chunk], swap_recv.at[chunk], partner
        )

    def go(chunk, k, sender):
        peer = lax.rem(chip + k, chips)
        slot = chip if sender else peer
        return remote(
            stage.at[chunk, peer], inbox.at[chunk, slot],
            go_send.at[chunk, k], go_recv.at[chunk, slot], mate(k),
        )

    def up(chunk, k, slot):
        return remote(
            total.at[chunk], earlier.at[chunk, slot],
            up_send.at[chunk, k], up_recv.at[chunk, slot], counter(k),
        )

    def give(chunk, k, sender):
        peer = lax.rem(chip + k, chips)
        slot = chip if sender else peer
        return remote(
            back.at[chunk, peer], prefix.at[chunk, slot], back_send.at[chunk, k], back_recv.at[chunk, slot], mate(k)
        )

    def hand(chunk):
        return remote(
            handed.at[chunk], received.at[chunk], hand_send.at[chunk], hand_recv.at[chunk], partner
        )

    first = side == 0
    mine_at = pl.ds(pl.multiple_of(side * half, half), half)

    def combine(chunk):
        swap_sides(chunk).wait_recv()
        a, b = own[chunk, mine_at, :CHUNK], other[chunk, :, :CHUNK]
        fa, fb = own[chunk, mine_at, CHUNK:], other[chunk, :, CHUNK:]
        late = across(jnp.where(first, fb, fa))
        both = late * jnp.where(first, a, b) + jnp.where(first, b, a)
        for p in range(chips):
            stage[chunk, p, :, :CHUNK] = both[p * piece : (p + 1) * piece]
            stage[chunk, p, :, CHUNK:] = (fa * fb)[p * piece : (p + 1) * piece]
        for k in range(1, chips):
            go(chunk, k, True).start()
        inbox[chunk, chip] = stage[chunk, chip]

    def give_all(chunk):
        for k in range(1, chips):
            give(chunk, k, True).start()
        prefix[chunk, chip] = back[chunk, chip]

    def scan_group(chunk):
        for k in range(1, chips):
            go(chunk, k, False).wait_recv()
        running = jnp.zeros((piece, CHUNK), jnp.float32)
        factor = jnp.ones((piece, LANES), jnp.float32)
        for m in range(chips):
            back[chunk, m] = running
            by = inbox[chunk, m, :, CHUNK:]
            spread[chunk, m] = factor
            running = across(by) * running + inbox[chunk, m, :, :CHUNK]
            factor = factor * by
        total[chunk, :, :CHUNK] = running
        total[chunk, :, CHUNK:] = factor
        for k in range(1, groups):

            @pl.when(group + k < groups)
            def _():
                up(chunk, k, group).start()

        @pl.when(group == 0)
        def _():
            give_all(chunk)

    def finish_groups(chunk):
        if groups == 1:
            return
        carried[...] = jnp.zeros((piece, CHUNK), jnp.float32)
        for g in range(groups - 1):

            @pl.when(g < group)
            def _():
                up(chunk, 1, g).wait_recv()
                by = earlier[chunk, g, :, CHUNK:]
                carried[...] = across(by) * carried[...] + earlier[chunk, g, :, :CHUNK]

        @pl.when(group > 0)
        def _():
            before = carried[...]
            for k in range(1, chips):
                peer = lax.rem(chip + k, chips)
                back[chunk, peer] += across(spread[chunk, peer]) * before
                give(chunk, k, True).start()
            prefix[chunk, chip] = back[chunk, chip] + across(spread[chunk, chip]) * before

    def write(chunk, which, values):
        at = pl.ds(pl.multiple_of((2 * chunk + which) * ROWS, ROWS), ROWS)
        for j in range(COLS // CHUNK):
            out_ref[at, j * CHUNK : (j + 1) * CHUNK] = values[j * ROWS : (j + 1) * ROWS]

    def pass_on(chunk):
        for k in range(1, chips):
            give(chunk, k, False).wait_recv()
        before = prefix[chunk].reshape(half, CHUNK)
        a, b = own[chunk, mine_at, :CHUNK], other[chunk, :, :CHUNK]
        fa, fb = own[chunk, mine_at, CHUNK:], other[chunk, :, CHUNK:]
        after = across(jnp.where(first, fa, fb)) * before + jnp.where(first, a, b)
        handed[chunk] = jnp.where(first, after, before)
        hand(chunk).start()
        write(chunk, side, jnp.where(first, before, after))

    def take(chunk):
        hand(chunk).wait_recv()
        write(chunk, 1 - side, received[chunk])

    for p in range(2):
        for w in range(windows):
            bins.multiply(w, p)
    bins.settle_first()
    pl.semaphore_wait(barrier, len(peers))
    swap_sides(0).start()
    for w in range(windows):
        if w == windows - 1:
            combine(0)
        bins.multiply(w, 2)
    bins.settle_second()
    swap_sides(1).start()
    bins.close()
    combine(1)
    for chunk in range(chunks):
        scan_group(chunk)
        if chunk == 0:
            finish_groups(chunk)
    for chunk in range(1, chunks):
        finish_groups(chunk)
    for chunk in range(chunks):
        pass_on(chunk)
    for chunk in range(chunks):
        take(chunk)

    for chunk in range(chunks):
        swap_sides(chunk).wait_send()
        hand(chunk).wait_send()
        for k in range(1, chips):
            go(chunk, k, True).wait_send()
            give(chunk, k, True).wait_send()
        for k in range(1, groups):

            @pl.when(group + k < groups)
            def _():
                up(chunk, k, group).wait_send()


def before_own(n, place, where_, weigh, spare, fact):
    windows = spare.shape[0]
    size = max(s for s in range(2, 2 * SLOTS // (2 * SUB) + 1, 2) if n % s == 0 and SLOTS % (s * SUB) == 0)
    groups, chips = n // size, size // 2
    half, chunks = COLS // CHUNK * ROWS, IMAGE_LAYERS // 2
    piece = half // chips
    wide = CHUNK + LANES
    dma = pltpu.SemaphoreType.DMA
    f32 = lambda *shape: pltpu.VMEM(shape, jnp.float32)
    return pl.pallas_call(
        functools.partial(scan_kernel, n, size),
        out_shape=(
            jax.ShapeDtypeStruct((windows, SLOTS, COLS), jnp.float32),
            jax.ShapeDtypeStruct((SLOTS, COLS), jnp.float32),
        ),
        in_specs=[pl.BlockSpec(memory_space=pltpu.VMEM)] * 5,
        out_specs=[pl.BlockSpec(memory_space=pltpu.VMEM)] * 2,
        scratch_shapes=[
            pltpu.VMEM((2, 256, 256), jnp.bfloat16),
            f32(chunks, 2 * half, wide), f32(chunks, half, wide), f32(chunks, chips, piece, wide),
            f32(chunks, chips, piece, wide), f32(chunks, piece, wide), f32(chunks, groups, piece, wide),
            f32(piece, CHUNK), f32(chunks, chips, piece, LANES), f32(chunks, chips, piece, CHUNK),
            f32(chunks, chips, piece, CHUNK), f32(chunks, half, CHUNK), f32(chunks, half, CHUNK),
            dma((chunks,)), dma((chunks,)), dma((chunks, chips)), dma((chunks, chips)),
            dma((chunks, groups)), dma((chunks, groups)), dma((chunks, chips)), dma((chunks, chips)),
            dma((chunks,)), dma((chunks,)),
        ],
        compiler_params=pltpu.CompilerParams(collective_id=0, has_side_effects=True, vmem_limit_bytes=16 * 2**20),
    )(place, where_, weigh, spare, fact)


def heat_kernel(running_ref, before_ref, fact_ref, out_hbm, out_ref, sem):
    windows = running_ref.shape[0]
    stores = []
    for channel in range(IMAGE_LAYERS):
        at = slice(channel * ROWS, (channel + 1) * ROWS)
        for window in range(windows):
            factor = jnp.concatenate([fact_ref[window, channel : channel + 1, :]] * (COLS // LANES), axis=1)
            out_ref[window, at] = factor * before_ref[at] + running_ref[window, at]
            stores.append(
                pltpu.make_async_copy(out_ref.at[window, at], out_hbm.at[window, at], sem.at[window, channel])
            )
            stores[-1].start()
    for store in stores:
        store.wait()


def heat(running, before, fact):
    windows = running.shape[0]
    return pl.pallas_call(
        heat_kernel,
        out_shape=jax.ShapeDtypeStruct(running.shape, jnp.float32),
        in_specs=[pl.BlockSpec(memory_space=pltpu.VMEM)] * 3,
        out_specs=pl.BlockSpec(memory_space=pltpu.HBM),
        scratch_shapes=[pltpu.VMEM(running.shape, jnp.float32), pltpu.SemaphoreType.DMA((windows, IMAGE_LAYERS))],
        compiler_params=pltpu.CompilerParams(vmem_limit_bytes=8 * 2**20),
    )(running, before, fact)


def local(n, point_rows, point_cols, point_chans, point_weights, decay):
    *points, fact = binned(point_rows, point_cols, point_chans, point_weights, decay)
    running, before = before_own(n, *points, fact)
    return heat(running, before, fact).reshape(-1, IMAGE_LAYERS, ROWS, COLS)


def solution(mesh):
    placed = (P("win", None),) * 5
    return jax.shard_map(
        functools.partial(local, mesh.shape["win"]),
        mesh=mesh, in_specs=placed, out_specs=P("win", None, None, None), check_vma=False,
    )
```
